128 devices in a mesh: pb: 4 (over z_hi, core), ka: 32 (over x, y, z_lo).
Axes of the slice: x: 4, y: 4, z: 4 (z_hi: 2, z_lo: 2; z = z_hi * 2 + z_lo), core: 2. Of those that a mesh axis runs over, the one named last changes fastest.
Arguments:
- queries: bfloat16 [16384, 1024], P(('pb', 'ka')), may hold values from -6 to 6
- key_rows: bfloat16 [16384, 128], P(('pb', 'ka')), may hold values from -6 to 6
- value_rows: bfloat16 [16384, 128], P(('pb', 'ka')), may hold values from -6 to 6
- forward_out: bfloat16 [16384, 1024], P(('pb', 'ka')), may hold values from -6 to 6
- out_grad: bfloat16 [16384, 1024], P(('pb', 'ka')), may hold values from -4 to 4
- logsumexp: float32 [8, 16384], P(None, ('pb', 'ka')), may hold values from 3 to 7
- position: int32 [16384], P(('pb', 'ka')), may hold values from 0 to 16383, as said below
- segment: int32 [16384], P(('pb', 'ka')), may hold values from 0 to 7, as said below
Outputs:
- query_grad: bfloat16 [16384, 1024], P(('pb', 'ka'))
- key_grad: bfloat16 [16384, 128], P(('pb', 'ka'))
- value_grad: bfloat16 [16384, 128], P(('pb', 'ka'))
The draws below stay inside these ranges and needn't reach their ends.
Inputs may be any that keep to these rules, and one draw needn't show every extreme that they name: `position`: a permutation of 0 to 16383; each aligned run of 128 rows holds 128 consecutive positions in increasing order. `segment`: the document of the row's position; each document is a nonempty run of consecutive positions, numbered in the order of positions, 8 documents in all.
All inputs are finite; a program needn't handle non-finite values.
Results may differ from the reference program's by a relative error of at most 0.0051.
Values may be sent and summed in bfloat16 or wider, within the bound.
A program may use at most 64 MiB of HBM per device.

```python
import jax
import jax.numpy as jnp
from jax import lax

HEADS = 8
HD = 128
TOK_DEV = 128
DOCS = 8
LENGTH = 16384


def build_layout(key):
    perm_key = jax.random.fold_in(key, 11)
    doc_key = jax.random.fold_in(key, 12)
    block_total = LENGTH // TOK_DEV
    block_order = jax.random.permutation(perm_key, block_total).astype(jnp.int32)
    position = (block_order[:, None] * TOK_DEV + jnp.arange(TOK_DEV, dtype=jnp.int32)[None, :]).reshape(-1).astype(jnp.int32)
    boundaries = (jax.random.choice(doc_key, LENGTH - 1, (DOCS - 1,), replace=False) + 1).astype(jnp.int32)
    document_ids = jnp.sum((jnp.arange(LENGTH, dtype=jnp.int32)[:, None] >= boundaries[None, :]).astype(jnp.int32), axis=1).astype(jnp.int32)
    segment = document_ids[position].astype(jnp.int32)
    return (position, segment)


def draw_position(key, part):
    return build_layout(key)[0]


def draw_segment(key, part):
    return build_layout(key)[1]


def level_of(own_key, dims, shards, least, largest):
    level, own = 1.0, jax.random.fold_in(own_key, 6)
    for dim, blocks in shards:
        steps = jnp.exp(jax.random.uniform(jax.random.fold_in(own, dim), (blocks,), jnp.float32, least / len(shards), largest / len(shards)))
        level = level * jnp.repeat(steps, dims[dim] // blocks).reshape([-1 if axis == dim else 1 for axis in range(len(dims))])
    return level


def centred(stream_key, extent, spread, reach, pieces=(), kind=jnp.bfloat16):
    entries = spread * jax.random.normal(stream_key, extent, jnp.float32)
    if pieces:
        entries = entries * level_of(stream_key, extent, pieces, -0.22, 0.18)
    return jnp.clip(entries, -reach, reach).astype(kind)


def setup_inputs(seed: int = 0) -> dict:
    seeds = jax.random.split(jax.random.key(seed), 9)
    return {
        "queries": centred(seeds[0], (LENGTH, HEADS * HD), 1.0, 6.0, ((0, 128),)),
        "key_rows": centred(seeds[1], (LENGTH, HD), 1.0, 6.0, ((0, 128),)),
        "value_rows": centred(seeds[2], (LENGTH, HD), 1.0, 6.0, ((0, 128),)),
        "forward_out": centred(seeds[3], (LENGTH, HEADS * HD), 0.5, 6.0, ((0, 128),)),
        "out_grad": centred(seeds[4], (LENGTH, HEADS * HD), 0.25, 4.0, ((0, 128),)),
        "logsumexp": jnp.clip(3.0 + 4.0 * jax.random.uniform(seeds[5], (HEADS, LENGTH), jnp.float32) ** level_of(seeds[5], (HEADS, LENGTH), ((1, 128),), -0.2, 0.2), 3.0, 7.0),
        "position": draw_position(jax.random.fold_in(seeds[8], 71), 0),
        "segment": draw_segment(jax.random.fold_in(seeds[8], 71), 0),
    }


def reference(queries, key_rows, value_rows, forward_out, out_grad, logsumexp, position, segment):
    head_width = key_rows.shape[1]
    row_count = queries.shape[0]
    head_count = queries.shape[1] // head_width
    score_scale = head_width ** -0.5
    highest = lax.Precision.HIGHEST
    delta_rows = jnp.sum((out_grad.astype(jnp.float32) * forward_out.astype(jnp.float32)).reshape(row_count, head_count, head_width), axis=2).T
    block_rows = min(512, row_count)
    block_count = row_count // block_rows
    key_float = key_rows.astype(jnp.float32)
    value_float = value_rows.astype(jnp.float32)

    def scan_step(loop_state, block_index):
        key_acc, value_acc = loop_state
        first_row = (block_index * block_rows).astype(jnp.int32)
        query_tile = lax.dynamic_slice_in_dim(queries, first_row, block_rows, 0).astype(jnp.float32).reshape(block_rows, head_count, head_width)
        grad_tile = lax.dynamic_slice_in_dim(out_grad, first_row, block_rows, 0).astype(jnp.float32).reshape(block_rows, head_count, head_width)
        lse_tile = lax.dynamic_slice_in_dim(logsumexp, first_row, block_rows, 1)
        delta_tile = lax.dynamic_slice_in_dim(delta_rows, first_row, block_rows, 1)
        place_tile = lax.dynamic_slice_in_dim(position, first_row, block_rows, 0)
        doc_tile = lax.dynamic_slice_in_dim(segment, first_row, block_rows, 0)
        visible = (position[None, :] <= place_tile[:, None]) & (segment[None, :] == doc_tile[:, None])
        scores = jnp.einsum("qhd,kd->hqk", query_tile, key_float, precision=highest) * score_scale
        weights = jnp.where(visible[None], jnp.exp(scores - lse_tile[:, :, None]), 0.0)
        rounded = lax.optimization_barrier(weights.astype(jnp.bfloat16)).astype(jnp.float32)
        value_acc = value_acc + jnp.einsum("hqk,qhd->kd", rounded, grad_tile, precision=highest)
        grad_scores = jnp.einsum("qhd,kd->hqk", grad_tile, value_float, precision=highest)
        score_grads = lax.optimization_barrier((weights * (grad_scores - delta_tile[:, :, None])).astype(jnp.bfloat16)).astype(jnp.float32)
        query_part = jnp.einsum("hqk,kd->qhd", score_grads, key_float, precision=highest).reshape(block_rows, head_count * head_width) * score_scale
        key_acc = key_acc + jnp.einsum("hqk,qhd->kd", score_grads, query_tile, precision=highest)
        return (key_acc, value_acc), query_part.astype(jnp.bfloat16)

    starting = (jnp.zeros((row_count, head_width), jnp.float32), jnp.zeros((row_count, head_width), jnp.float32))
    (key_acc, value_acc), grad_blocks = lax.scan(scan_step, starting, jnp.arange(block_count, dtype=jnp.int32))
    query_grad = grad_blocks.reshape(row_count, head_count * head_width)
    return query_grad, (key_acc * score_scale).astype(jnp.bfloat16), value_acc.astype(jnp.bfloat16)
```

```python
import functools

import jax
import jax.numpy as jnp
from jax import lax
from jax.experimental import pallas as pl
from jax.experimental.pallas import tpu as pltpu
from jax.sharding import PartitionSpec as P

MESH = pl.DeviceIdType.MESH
F32 = jnp.float32
BF16 = jnp.bfloat16
SIDE = 4
HEADS = 8
HD = 128
TOK = 128
GROUP = 2 * SIDE * SIDE
QS = 4
KVR = 272
STR = 24
DOCS = 8
FAR = 1 << 20
LOG2E = 1.4426950408889634


class Place:
    def __init__(self):
        pb, ka = lax.axis_index("pb"), lax.axis_index("ka")
        self.c, self.zh = lax.rem(pb, 2), pb // 2
        self.zl, u = lax.rem(ka, 2), ka // 2
        self.x, self.y = u // SIDE, lax.rem(u, SIDE)
        self.z = self.zh * 2 + self.zl
        self.half = (1 - self.zl, self.zl)
        self.sib = self.dev(self.x, self.y, self.z, 1 - self.c)
        self.zq = self.dev(self.x, self.y, self.zh * 2 + 1 - self.zl, self.c)
        self.zk = self.dev(self.x, self.y, lax.rem(self.z + 3 + 2 * self.zl, SIDE), self.c)

    def dev(self, x, y, z, c):
        return {"pb": (z // 2) * 2 + c, "ka": (x * SIDE + y) * 2 + lax.rem(z, 2)}

    def moved(self, w, dp, ds):
        hw = self.half[w]
        x = lax.rem(self.x + SIDE + dp * (1 - hw) + ds * hw, SIDE)
        y = lax.rem(self.y + SIDE + dp * hw + ds * (1 - hw), SIDE)
        return x, y

    def nbr(self, w, dp, ds):
        x, y = self.moved(w, dp, ds)
        return self.dev(x, y, self.z, self.c)

    def slot(self, w, dp, ds):
        x, y = self.moved(w, dp, ds)
        return (x * SIDE + y) * 2 + self.half[w]

    def greet(self):
        partners = [
            self.sib,
            self.zq,
            self.zk,
            self.nbr(0, 1, 0),
            self.nbr(0, -1, 0),
            self.nbr(0, 0, 1),
            self.nbr(0, 0, -1),
        ]
        barrier = pltpu.get_barrier_semaphore()
        for partner in partners:
            pl.semaphore_signal(barrier, inc=1, device_id=partner, device_id_type=MESH)
        pl.semaphore_wait(barrier, len(partners))


def remote(src, dst, send_sem, recv_sem, device):
    return pltpu.make_async_remote_copy(
        src_ref=src,
        dst_ref=dst,
        send_sem=send_sem,
        recv_sem=recv_sem,
        device_id=device,
        device_id_type=MESH,
    )


def gather_kernel(
    q_in, k_in, v_in, o_in, g_in, lse_in, pos_in, seg_in,
    q_all, g_all, st_all, kv_all,
    o_buf, lse_buf, pos_buf, seg_buf, loc, ksend, krecv, qsend, qrecv,
):
    at = Place()
    slot = at.slot(0, 0, 0)
    qslot = at.zl * 2 + at.c
    local = [
        pltpu.make_async_copy(k_in, kv_all.at[slot, pl.ds(0, TOK)], loc.at[0]),
        pltpu.make_async_copy(v_in, kv_all.at[slot, pl.ds(TOK, TOK)], loc.at[1]),
        pltpu.make_async_copy(q_in, q_all.at[qslot], loc.at[2]),
        pltpu.make_async_copy(g_in, g_all.at[qslot], loc.at[3]),
        pltpu.make_async_copy(o_in, o_buf, loc.at[4]),
        pltpu.make_async_copy(lse_in, lse_buf, loc.at[5]),
        pltpu.make_async_copy(pos_in, pos_buf, loc.at[6]),
        pltpu.make_async_copy(seg_in, seg_buf, loc.at[7]),
    ]
    for copy in (local[6], local[7], *local[:6]):
        copy.start()
    at.greet()
    local[6].wait()
    local[7].wait()
    seg = seg_buf[...].astype(F32)
    pos = pos_buf[...].astype(F32)
    row = lax.broadcasted_iota(jnp.int32, (16, TOK), 0)
    block_number = (pos_buf[...] // TOK).astype(F32)
    kv_all[slot, pl.ds(2 * TOK, 16), :] = jnp.where(row == 0, seg, block_number).astype(BF16)
    sends = []

    def kv_copy(w, index, where, r0, rows, device):
        part = kv_all.at[where, pl.ds(r0, rows)]
        n = 20 * w + index
        return remote(part, part, ksend.at[n], krecv.at[n], device)

    def go(copy):
        copy.start()
        sends.append(copy)

    WHOLE, KEYS, REST = (0, KVR), (0, TOK), (TOK, KVR - TOK)
    order = (0, -1, 1, 2)

    def stage_one(w):
        go(kv_copy(w, 0, at.slot(w, 0, 0), *WHOLE, at.nbr(w, 1, 0)))
        go(kv_copy(w, 1, at.slot(w, 0, 0), *WHOLE, at.nbr(w, -1, 0)))

    def direct(w, j):
        here = at.slot(w, order[j], 0)
        go(kv_copy(w, 4 + 2 * j, here, *WHOLE, at.nbr(w, 0, 1)))
        go(kv_copy(w, 5 + 2 * j, here, *WHOLE, at.nbr(w, 0, -1)))

    def direct_arrived(w, j):
        kv_copy(w, 4 + 2 * j, at.slot(w, order[j], -1), *WHOLE, at.nbr(w, 0, 1)).wait_recv()
        go(kv_copy(w, 12 + 2 * j, at.slot(w, order[j], -1), *KEYS, at.nbr(w, 0, 1)))
        kv_copy(w, 5 + 2 * j, at.slot(w, order[j], 1), *WHOLE, at.nbr(w, 0, 1)).wait_recv()
        go(kv_copy(w, 13 + 2 * j, at.slot(w, order[j], 1), *REST, at.nbr(w, 0, -1)))

    local[0].wait()
    local[1].wait()
    part = kv_all.at[slot]
    go(remote(part, part, ksend.at[40], krecv.at[40], at.zk))
    stage_one(0)
    direct(0, 0)

    def piece(who, n):
        if n < 4:
            ref = q_all if n < 2 else g_all
            return ref.at[who, pl.ds((n % 2) * (TOK // 2), TOK // 2)]
        return st_all.at[who]

    def q_copy(kind, n, who, device):
        part = piece(who, n)
        return remote(part, part, qsend.at[5 * kind + n], qrecv.at[5 * kind + n], device)

    local[2].wait()
    for n in (0, 1):
        go(q_copy(0, n, qslot, at.zq))
    local[3].wait()
    for n in (2, 3):
        go(q_copy(0, n, qslot, at.zq))
    for n in range(4):
        go(q_copy(1, n, qslot, at.sib))

    other = at.slot(1, 0, 0)
    part = kv_all.at[other]
    remote(part, part, ksend.at[40], krecv.at[40], at.zk).wait_recv()
    stage_one(1)
    direct(1, 0)

    local[4].wait()
    local[5].wait()
    st_all[qslot, pl.ds(0, HEADS), :] = lse_buf[...]
    for h in range(HEADS):
        cols = pl.ds(h * HD, HD)
        prod = g_all[qslot, :, cols].astype(F32) * o_buf[:, cols].astype(F32)
        st_all[qslot, pl.ds(HEADS + h, 1), :] = jnp.sum(prod.T, axis=0, keepdims=True)
    row = lax.broadcasted_iota(jnp.int32, (8, TOK), 0)
    st_all[qslot, pl.ds(16, 8), :] = jnp.where(row == 0, seg, pos)

    for w in (0, 1):
        kv_copy(w, 0, at.slot(w, -1, 0), *WHOLE, at.nbr(w, 1, 0)).wait_recv()
        go(kv_copy(w, 2, at.slot(w, -1, 0), *KEYS, at.nbr(w, 1, 0)))
        kv_copy(w, 1, at.slot(w, 1, 0), *WHOLE, at.nbr(w, 1, 0)).wait_recv()
        go(kv_copy(w, 3, at.slot(w, 1, 0), *REST, at.nbr(w, -1, 0)))
    for w in (0, 1):
        direct(w, 1)
        direct(w, 2)
    go(q_copy(0, 4, qslot, at.zq))
    go(q_copy(1, 4, qslot, at.sib))
    for w in (0, 1):
        direct_arrived(w, 0)
    for w in (0, 1):
        kv_copy(w, 2, at.slot(w, -2, 0), *KEYS, at.nbr(w, 1, 0)).wait_recv()
        kv_copy(w, 3, at.slot(w, 2, 0), *REST, at.nbr(w, 1, 0)).wait_recv()
        direct(w, 3)
    far = (1 - at.zl) * 2 + at.c

    def pass_on(n):
        q_copy(0, n, far, at.zq).wait_recv()
        go(q_copy(2, n, far, at.sib))

    for j in (1, 2, 3):
        for w in (0, 1):
            direct_arrived(w, j)
        pass_on(j - 1)
    pass_on(3)
    pass_on(4)
    for j in range(4):
        for w in (0, 1):
            kv_copy(w, 12 + 2 * j, at.slot(w, order[j], -2), *KEYS, at.nbr(w, 0, 1)).wait_recv()
            kv_copy(w, 13 + 2 * j, at.slot(w, order[j], 2), *REST, at.nbr(w, 0, 1)).wait_recv()
    for n in range(5):
        q_copy(1, n, at.zl * 2 + 1 - at.c, at.sib).wait_recv()
        q_copy(2, n, (1 - at.zl) * 2 + 1 - at.c, at.sib).wait_recv()
    for copy in sends:
        copy.wait_send()


def grads_kernel(
    q_ref, g_ref, st_ref, kv_ref, dq_ref, dkv_ref,
    listed, low_ref, base_ref, bias_ref, w_buf, s_buf,
):
    dq_ref[...] = jnp.zeros_like(dq_ref)
    dkv_ref[...] = jnp.zeros_like(dkv_ref)

    tail = kv_ref[:, pl.ds(2 * TOK, 16), :].astype(F32)
    key_doc = tail[:, 0, :].astype(jnp.int32)
    key_base = tail[:, 1, :].astype(jnp.int32) * TOK
    base_ref[...] = key_base
    lane = lax.broadcasted_iota(jnp.int32, (GROUP, TOK), 1)
    key_place = key_base + lane
    query_doc = jnp.concatenate([st_ref[i, pl.ds(16, 1), :] for i in range(QS)], axis=0)
    query_doc = query_doc.astype(jnp.int32)
    query_place = jnp.concatenate([st_ref[i, pl.ds(17, 1), :] for i in range(QS)], axis=0)
    query_place = query_place.astype(jnp.int32)
    low = jnp.full((QS, TOK), FAR, jnp.int32)
    for d in range(DOCS):
        first = jnp.min(jnp.where(key_doc == d, key_place, FAR))
        low = jnp.where(query_doc == d, first, low)
    low_ref[pl.ds(0, QS), :] = low
    low_ref[pl.ds(QS, QS), :] = query_place
    key_row = lax.broadcasted_iota(jnp.int32, (GROUP, TOK), 0)
    count = jnp.int32(0)
    for i in range(QS):
        top = jnp.max(query_place[i : i + 1])
        least = jnp.min(low[i : i + 1])
        active = (key_base <= top) & (key_base + (TOK - 1) >= least)
        for part in range(2):
            bits = jnp.where(
                active & (key_row // 16 == part), jnp.left_shift(1, lax.rem(key_row, 16)), 0
            )
            word = jnp.max(jnp.sum(bits, axis=0, keepdims=True))

            def note(j, count, i=i, part=part, word=word):
                listed[count] = i * 64 + (part * 16 + j) * 2 + 1
                return count + (lax.shift_right_logical(word, j) & 1)

            count = lax.fori_loop(0, 16, note, count)
        last = listed[jnp.maximum(count - 1, 0)]
        listed[count] = last & -2
        count = count + (count & 1)

    sublane = lax.broadcasted_iota(jnp.int32, (TOK, TOK), 0)
    score_scale = HD ** (-0.5) * LOG2E
    nt = (((1,), (1,)), ((), ()))

    def over_pairs(pair, carry):
        one, two = listed[2 * pair], listed[2 * pair + 1]
        i = one // 64
        k0 = lax.rem(one // 2, GROUP)
        k1 = lax.rem(two // 2, GROUP)
        lo, hi = low_ref[pl.ds(i, 1), :], low_ref[pl.ds(QS + i, 1), :]
        b0, b1 = base_ref[pl.ds(k0, 1), :], base_ref[pl.ds(k1, 1), :]
        hi1 = jnp.where((two & 1) == 1, hi - b1, -1)
        bias_ref[pl.ds(0, TOK), :] = jnp.where(
            (sublane >= lo - b0) & (sublane <= hi - b0), 0.0, -1e30
        )
        bias_ref[pl.ds(TOK, TOK), :] = jnp.where(
            (sublane >= lo - b1) & (sublane <= hi1), 0.0, -1e30
        )
        kk = jnp.concatenate([kv_ref[k0, pl.ds(0, TOK), :], kv_ref[k1, pl.ds(0, TOK), :]], axis=0)
        vv = jnp.concatenate(
            [kv_ref[k0, pl.ds(TOK, TOK), :], kv_ref[k1, pl.ds(TOK, TOK), :]], axis=0
        )
        kt = kk.T

        def heads(ref, hp):
            a = ref[i, :, pl.ds(2 * hp * HD, HD)]
            b = ref[i, :, pl.ds((2 * hp + 1) * HD, HD)]
            return jnp.concatenate([a, b], axis=0)

        def rows(first, hp):
            a = st_ref[i, pl.ds(first + 2 * hp, 1), :]
            b = st_ref[i, pl.ds(first + 2 * hp + 1, 1), :]
            return jnp.concatenate([a, b], axis=1)

        for hp in range(HEADS // 2):
            cols = pl.ds(2 * hp * HD, 2 * HD)
            scores = lax.dot_general(kk, heads(q_ref, hp), nt, preferred_element_type=F32)
            bias = bias_ref[...]
            bias = jnp.concatenate([bias, bias], axis=1)
            weights = jnp.exp2(scores * score_scale + (bias - rows(0, hp) * LOG2E))
            w_buf[:, cols] = weights.astype(BF16)
            grads = lax.dot_general(vv, heads(g_ref, hp), nt, preferred_element_type=F32)
            score_grads = (weights * (grads - rows(HEADS, hp))).astype(BF16)
            s_buf[:, cols] = score_grads
            dq_ref[i, :, cols] += jnp.dot(kt, score_grads, preferred_element_type=F32)
        stack_g = jnp.concatenate([g_ref[i, :, pl.ds(h * HD, HD)] for h in range(HEADS)], axis=0)
        stack_q = jnp.concatenate([q_ref[i, :, pl.ds(h * HD, HD)] for h in range(HEADS)], axis=0)
        dv = jnp.dot(w_buf[...], stack_g, preferred_element_type=F32)
        dk = jnp.dot(s_buf[...], stack_q, preferred_element_type=F32)
        dkv_ref[k0, pl.ds(0, TOK), :] += dk[:TOK]
        dkv_ref[k0, pl.ds(TOK, TOK), :] += dv[:TOK]
        dkv_ref[k1, pl.ds(0, TOK), :] += dk[TOK:]
        dkv_ref[k1, pl.ds(TOK, TOK), :] += dv[TOK:]
        return carry

    lax.fori_loop(0, count // 2, over_pairs, 0)


def reduce_kernel(
    dq_ref, dkv_ref,
    dq_out, dk_out, dv_out,
    out1, in1, out2, in2, out3, in3, part1, mine, near, sibq, farq_out, farq_in,
    s1, r1, s2, r2, s3, r3, sq, rq,
):
    at = Place()
    score_scale = HD ** (-0.5)
    sends = []

    def go(copy):
        copy.start()
        sends.append(copy)

    at.greet()
    qslot = at.zl * 2 + at.c
    sib_far = (1 - at.zl) * 2 + 1 - at.c
    sib_own = at.zl * 2 + 1 - at.c
    my_far = (1 - at.zl) * 2 + at.c
    CH = HD // 4

    def far_piece(n):
        rows = pl.ds(n * CH, CH)
        return remote(dq_ref.at[sib_far, rows], near.at[rows], sq.at[n], rq.at[n], at.sib)

    def far_send(n):
        rows = pl.ds(n * CH, CH)
        return remote(farq_out.at[rows], farq_in.at[rows], sq.at[4 + n], rq.at[4 + n], at.zq)

    own_piece = remote(dq_ref.at[sib_own], sibq, sq.at[8], rq.at[8], at.sib)
    for n in range(4):
        go(far_piece(n))
    go(own_piece)

    order = (2, 1, -1, 0)
    K, V = pl.ds(0, HD), pl.ds(HD, HD)

    def hop1(w, j, t):
        ahead = 1 if t % 2 == 0 else -1
        n = (w * 4 + j) * 6 + t
        return remote(
            out1.at[n], in1.at[n], s1.at[n], r1.at[n], at.nbr(w, 0, ahead)
        )

    def hop2(w, t):
        ahead = 1 if t % 2 == 0 else -1
        n = w * 6 + t
        return remote(out2.at[n], in2.at[n], s2.at[n], r2.at[n], at.nbr(w, ahead, 0))

    def first(w, j, t):
        dp = order[j]
        where = (2, 2, 1, -1)[t]
        rows = (K, V, V, K)[t]
        out1[(w * 4 + j) * 6 + t] = dkv_ref[at.slot(w, dp, where), rows, :].astype(BF16)
        go(hop1(w, j, t))

    for t in (0, 1):
        for j in range(4):
            for w in (1, 0):
                first(w, j, t)
    for n in range(4):
        rows = pl.ds(n * CH, CH)
        far_piece(n).wait_recv()
        farq_out[rows, :] = (dq_ref[my_far, rows, :] + near[rows, :]).astype(BF16)
        go(far_send(n))
    for t in (2, 3):
        for j in range(4):
            for w in (1, 0):
                first(w, j, t)
    for j in range(4):
        for w in (1, 0):
            base = (w * 4 + j) * 6
            for t, where, rows in ((4, 1, K), (5, -1, V)):
                hop1(w, j, t - 4).wait_recv()
                own = dkv_ref[at.slot(w, order[j], where), rows, :]
                out1[base + t] = (own + in1[base + t - 4].astype(F32)).astype(BF16)
                go(hop1(w, j, t))

    def settle(w, j):
        base = (w * 4 + j) * 6
        for t in (2, 3, 4, 5):
            hop1(w, j, t).wait_recv()
        own = dkv_ref[at.slot(w, order[j], 0)]
        dk = own[:HD] + in1[base + 3].astype(F32) + in1[base + 4].astype(F32)
        dv = own[HD:] + in1[base + 2].astype(F32) + in1[base + 5].astype(F32)
        return dk, dv

    def second(w, t, value):
        out2[w * 6 + t] = value.astype(BF16)
        go(hop2(w, t))

    for w in (1, 0):
        dk, dv = settle(w, 0)
        second(w, 0, dk)
        second(w, 1, dv)
    for w in (1, 0):
        dk, dv = settle(w, 1)
        part1[w, 0] = dk
        second(w, 2, dv)
        dk, dv = settle(w, 2)
        part1[w, 1] = dv
        second(w, 3, dk)
    for w in (1, 0):
        hop2(w, 0).wait_recv()
        second(w, 4, part1[w, 0] + in2[w * 6].astype(F32))
        hop2(w, 1).wait_recv()
        second(w, 5, part1[w, 1] + in2[w * 6 + 1].astype(F32))

    def total(w):
        dk, dv = settle(w, 3)
        for t in (2, 3, 4, 5):
            hop2(w, t).wait_recv()
        base = w * 6
        dk = dk + in2[base + 3].astype(F32) + in2[base + 4].astype(F32)
        dv = dv + in2[base + 2].astype(F32) + in2[base + 5].astype(F32)
        return dk, dv

    across = remote(out3, in3, s3.at[0], r3.at[0], at.zk)
    dk, dv = total(1)
    out3[0] = dk.astype(BF16)
    out3[1] = dv.astype(BF16)
    go(across)
    dk, dv = total(0)
    mine[0] = dk
    mine[1] = dv
    own_piece.wait_recv()
    for n in range(4):
        far_send(n).wait_recv()
    for h in range(HEADS):
        cols = pl.ds(h * HD, HD)
        value = dq_ref[qslot, :, cols] + sibq[:, cols] + farq_in[:, cols].astype(F32)
        dq_out[:, cols] = (value * score_scale).T.astype(BF16)
    across.wait_recv()
    dk_out[...] = ((mine[0] + in3[0].astype(F32)) * score_scale).astype(BF16)
    dv_out[...] = (mine[1] + in3[1].astype(F32)).astype(BF16)
    for copy in sends:
        copy.wait_send()


HB = pl.BlockSpec(memory_space=pltpu.HBM)
VM = pl.BlockSpec(memory_space=pltpu.VMEM)
DMA = pltpu.SemaphoreType.DMA


def gather(queries, key_rows, value_rows, forward_out, out_grad, logsumexp, position, segment):
    wide = HEADS * HD
    args = (
        queries, key_rows, value_rows, forward_out, out_grad,
        logsumexp, position.reshape(1, TOK), segment.reshape(1, TOK),
    )
    return pl.pallas_call(
        gather_kernel,
        out_shape=(
            pltpu.VMEM((QS, TOK, wide), BF16),
            pltpu.VMEM((QS, TOK, wide), BF16),
            pltpu.VMEM((QS, STR, TOK), F32),
            pltpu.VMEM((GROUP, KVR, HD), BF16),
        ),
        in_specs=[HB] * 8,
        out_specs=(VM,) * 4,
        scratch_shapes=[
            pltpu.VMEM((TOK, wide), BF16),
            pltpu.VMEM((HEADS, TOK), F32),
            pltpu.VMEM((1, TOK), jnp.int32),
            pltpu.VMEM((1, TOK), jnp.int32),
            DMA((8,)),
            DMA((41,)),
            DMA((41,)),
            DMA((15,)),
            DMA((15,)),
        ],
        compiler_params=pltpu.CompilerParams(
            collective_id=0, has_side_effects=True, vmem_limit_bytes=8 << 20
        ),
        name="gather_rows",
    )(*[pltpu.with_memory_space_constraint(a, pltpu.HBM) for a in args])


def grads(q_all, g_all, st_all, kv_all):
    wide = HEADS * HD
    return pl.pallas_call(
        grads_kernel,
        out_shape=(
            pltpu.VMEM((QS, HD, wide), F32),
            pltpu.VMEM((GROUP, 2 * HD, HD), F32),
        ),
        in_specs=[VM] * 4,
        out_specs=(VM,) * 2,
        scratch_shapes=[
            pltpu.SMEM((QS * GROUP + 16,), jnp.int32),
            pltpu.VMEM((2 * QS, TOK), jnp.int32),
            pltpu.VMEM((GROUP, TOK), jnp.int32),
            pltpu.VMEM((2 * TOK, TOK), F32),
            pltpu.VMEM((2 * TOK, wide), BF16),
            pltpu.VMEM((2 * TOK, wide), BF16),
        ],
        compiler_params=pltpu.CompilerParams(vmem_limit_bytes=24 << 20),
        name="tile_grads",
    )(q_all, g_all, st_all, kv_all)


def reduce(dq_all, dkv_all):
    wide = HEADS * HD
    return pl.pallas_call(
        reduce_kernel,
        out_shape=(
            jax.ShapeDtypeStruct((TOK, wide), BF16),
            jax.ShapeDtypeStruct((TOK, HD), BF16),
            jax.ShapeDtypeStruct((TOK, HD), BF16),
        ),
        in_specs=[VM] * 2,
        out_specs=(VM,) * 3,
        scratch_shapes=[
            pltpu.VMEM((48, HD, HD), BF16),
            pltpu.VMEM((48, HD, HD), BF16),
            pltpu.VMEM((12, HD, HD), BF16),
            pltpu.VMEM((12, HD, HD), BF16),
            pltpu.VMEM((2, HD, HD), BF16),
            pltpu.VMEM((2, HD, HD), BF16),
            pltpu.VMEM((2, 2, HD, HD), F32),
            pltpu.VMEM((2, HD, HD), F32),
            pltpu.VMEM((HD, wide), F32),
            pltpu.VMEM((HD, wide), F32),
            pltpu.VMEM((HD, wide), BF16),
            pltpu.VMEM((HD, wide), BF16),
            DMA((48,)), DMA((48,)), DMA((12,)), DMA((12,)), DMA((1,)), DMA((1,)), DMA((9,)), DMA((9,)),
        ],
        compiler_params=pltpu.CompilerParams(
            collective_id=1, has_side_effects=True, vmem_limit_bytes=24 << 20
        ),
        name="reduce_grads",
    )(dq_all, dkv_all)


def body(*args):
    return reduce(*grads(*gather(*args)))


def solution(mesh):
    rows = P(("pb", "ka"), None)
    flat = P(("pb", "ka"))
    placed = (rows,) * 5 + (P(None, ("pb", "ka")), flat, flat)
    return jax.shard_map(
        body, mesh=mesh, in_specs=placed, out_specs=(rows,) * 3, check_vma=False
    )
```

```python
import functools

import jax
import jax.numpy as jnp
from jax import lax
from jax.experimental import pallas as pl
from jax.experimental.pallas import tpu as pltpu
from jax.sharding import PartitionSpec as P

MESH = pl.DeviceIdType.MESH
F32 = jnp.float32
BF16 = jnp.bfloat16
SIDE = 4
HEADS = 8
HD = 128
TOK = 128
GROUP = 2 * SIDE * SIDE
QS = 4
KVR = 272
STR = 24
DOCS = 8
FAR = 1 << 20
LOG2E = 1.4426950408889634


class Place:
    def __init__(self):
        pb, ka = lax.axis_index("pb"), lax.axis_index("ka")
        self.c, self.zh = lax.rem(pb, 2), pb // 2
        self.zl, u = lax.rem(ka, 2), ka // 2
        self.x, self.y = u // SIDE, lax.rem(u, SIDE)
        self.z = self.zh * 2 + self.zl
        self.half = (1 - self.zl, self.zl)
        self.sib = self.dev(self.x, self.y, self.z, 1 - self.c)
        self.zq = self.dev(self.x, self.y, self.zh * 2 + 1 - self.zl, self.c)
        self.zk = self.dev(self.x, self.y, lax.rem(self.z + 3 + 2 * self.zl, SIDE), self.c)

    def dev(self, x, y, z, c):
        return {"pb": (z // 2) * 2 + c, "ka": (x * SIDE + y) * 2 + lax.rem(z, 2)}

    def moved(self, w, dp, ds):
        hw = self.half[w]
        x = lax.rem(self.x + SIDE + dp * (1 - hw) + ds * hw, SIDE)
        y = lax.rem(self.y + SIDE + dp * hw + ds * (1 - hw), SIDE)
        return x, y

    def nbr(self, w, dp, ds):
        x, y = self.moved(w, dp, ds)
        return self.dev(x, y, self.z, self.c)

    def slot(self, w, dp, ds):
        x, y = self.moved(w, dp, ds)
        return (x * SIDE + y) * 2 + self.half[w]

    def greet(self):
        partners = [
            self.sib,
            self.zq,
            self.zk,
            self.nbr(0, 1, 0),
            self.nbr(0, -1, 0),
            self.nbr(0, 0, 1),
            self.nbr(0, 0, -1),
        ]
        barrier = pltpu.get_barrier_semaphore()
        for partner in partners:
            pl.semaphore_signal(barrier, inc=1, device_id=partner, device_id_type=MESH)
        pl.semaphore_wait(barrier, len(partners))


def remote(src, dst, send_sem, recv_sem, device):
    return pltpu.make_async_remote_copy(
        src_ref=src,
        dst_ref=dst,
        send_sem=send_sem,
        recv_sem=recv_sem,
        device_id=device,
        device_id_type=MESH,
    )


def gather_kernel(
    q_in, k_in, v_in, o_in, g_in, lse_in, pos_in, seg_in,
    q_all, g_all, st_all, kv_all, dq_zero, dkv_zero,
    o_buf, lse_buf, pos_buf, seg_buf, loc, ksend, krecv, qsend, qrecv,
):
    at = Place()
    slot = at.slot(0, 0, 0)
    qslot = at.zl * 2 + at.c
    local = [
        pltpu.make_async_copy(k_in, kv_all.at[slot, pl.ds(0, TOK)], loc.at[0]),
        pltpu.make_async_copy(v_in, kv_all.at[slot, pl.ds(TOK, TOK)], loc.at[1]),
        pltpu.make_async_copy(q_in, q_all.at[qslot], loc.at[2]),
        pltpu.make_async_copy(g_in, g_all.at[qslot], loc.at[3]),
        pltpu.make_async_copy(o_in, o_buf, loc.at[4]),
        pltpu.make_async_copy(lse_in, lse_buf, loc.at[5]),
        pltpu.make_async_copy(pos_in, pos_buf, loc.at[6]),
        pltpu.make_async_copy(seg_in, seg_buf, loc.at[7]),
    ]
    for copy in (local[6], local[7], *local[:6]):
        copy.start()
    at.greet()
    local[6].wait()
    local[7].wait()
    seg = seg_buf[...].astype(F32)
    pos = pos_buf[...].astype(F32)
    row = lax.broadcasted_iota(jnp.int32, (16, TOK), 0)
    block_number = (pos_buf[...] // TOK).astype(F32)
    kv_all[slot, pl.ds(2 * TOK, 16), :] = jnp.where(row == 0, seg, block_number).astype(BF16)
    sends = []

    def kv_copy(w, index, where, r0, rows, device):
        part = kv_all.at[where, pl.ds(r0, rows)]
        n = 20 * w + index
        return remote(part, part, ksend.at[n], krecv.at[n], device)

    def go(copy):
        copy.start()
        sends.append(copy)

    WHOLE, KEYS, REST = (0, KVR), (0, TOK), (TOK, KVR - TOK)
    order = (0, -1, 1, 2)

    def stage_one(w):
        go(kv_copy(w, 0, at.slot(w, 0, 0), *WHOLE, at.nbr(w, 1, 0)))
        go(kv_copy(w, 1, at.slot(w, 0, 0), *WHOLE, at.nbr(w, -1, 0)))

    def direct(w, j):
        here = at.slot(w, order[j], 0)
        go(kv_copy(w, 4 + 2 * j, here, *WHOLE, at.nbr(w, 0, 1)))
        go(kv_copy(w, 5 + 2 * j, here, *WHOLE, at.nbr(w, 0, -1)))

    def direct_arrived(w, j):
        kv_copy(w, 4 + 2 * j, at.slot(w, order[j], -1), *WHOLE, at.nbr(w, 0, 1)).wait_recv()
        go(kv_copy(w, 12 + 2 * j, at.slot(w, order[j], -1), *KEYS, at.nbr(w, 0, 1)))
        kv_copy(w, 5 + 2 * j, at.slot(w, order[j], 1), *WHOLE, at.nbr(w, 0, 1)).wait_recv()
        go(kv_copy(w, 13 + 2 * j, at.slot(w, order[j], 1), *REST, at.nbr(w, 0, -1)))

    local[0].wait()
    local[1].wait()
    part = kv_all.at[slot]
    go(remote(part, part, ksend.at[40], krecv.at[40], at.zk))
    stage_one(0)
    direct(0, 0)

    def piece(who, n):
        if n < 4:
            ref = q_all if n < 2 else g_all
            return ref.at[who, pl.ds((n % 2) * (TOK // 2), TOK // 2)]
        return st_all.at[who]

    def q_copy(kind, n, who, device):
        part = piece(who, n)
        return remote(part, part, qsend.at[5 * kind + n], qrecv.at[5 * kind + n], device)

    local[2].wait()
    for n in (0, 1):
        go(q_copy(0, n, qslot, at.zq))
    local[3].wait()
    for n in (2, 3):
        go(q_copy(0, n, qslot, at.zq))
    for n in range(4):
        go(q_copy(1, n, qslot, at.sib))

    dq_zero[...] = jnp.zeros_like(dq_zero)
    other = at.slot(1, 0, 0)
    part = kv_all.at[other]
    remote(part, part, ksend.at[40], krecv.at[40], at.zk).wait_recv()
    stage_one(1)
    direct(1, 0)

    local[4].wait()
    local[5].wait()
    st_all[qslot, pl.ds(0, HEADS), :] = lse_buf[...]
    for h in range(HEADS):
        cols = pl.ds(h * HD, HD)
        prod = g_all[qslot, :, cols].astype(F32) * o_buf[:, cols].astype(F32)
        st_all[qslot, pl.ds(HEADS + h, 1), :] = jnp.sum(prod.T, axis=0, keepdims=True)
    row = lax.broadcasted_iota(jnp.int32, (8, TOK), 0)
    st_all[qslot, pl.ds(16, 8), :] = jnp.where(row == 0, seg, pos)

    for w in (0, 1):
        kv_copy(w, 0, at.slot(w, -1, 0), *WHOLE, at.nbr(w, 1, 0)).wait_recv()
        go(kv_copy(w, 2, at.slot(w, -1, 0), *KEYS, at.nbr(w, 1, 0)))
        kv_copy(w, 1, at.slot(w, 1, 0), *WHOLE, at.nbr(w, 1, 0)).wait_recv()
        go(kv_copy(w, 3, at.slot(w, 1, 0), *REST, at.nbr(w, -1, 0)))
    for w in (0, 1):
        direct(w, 1)
        direct(w, 2)
    go(q_copy(0, 4, qslot, at.zq))
    go(q_copy(1, 4, qslot, at.sib))
    dkv_zero[...] = jnp.zeros_like(dkv_zero)
    for w in (0, 1):
        direct_arrived(w, 0)
    for w in (0, 1):
        kv_copy(w, 2, at.slot(w, -2, 0), *KEYS, at.nbr(w, 1, 0)).wait_recv()
        kv_copy(w, 3, at.slot(w, 2, 0), *REST, at.nbr(w, 1, 0)).wait_recv()
        direct(w, 3)
    far = (1 - at.zl) * 2 + at.c

    def pass_on(n):
        q_copy(0, n, far, at.zq).wait_recv()
        go(q_copy(2, n, far, at.sib))

    for j in (1, 2, 3):
        for w in (0, 1):
            direct_arrived(w, j)
        pass_on(j - 1)
    pass_on(3)
    pass_on(4)
    for j in range(4):
        for w in (0, 1):
            kv_copy(w, 12 + 2 * j, at.slot(w, order[j], -2), *KEYS, at.nbr(w, 0, 1)).wait_recv()
            kv_copy(w, 13 + 2 * j, at.slot(w, order[j], 2), *REST, at.nbr(w, 0, 1)).wait_recv()
    for n in range(5):
        q_copy(1, n, at.zl * 2 + 1 - at.c, at.sib).wait_recv()
        q_copy(2, n, (1 - at.zl) * 2 + 1 - at.c, at.sib).wait_recv()
    for copy in sends:
        copy.wait_send()


def grads_kernel(
    q_ref, g_ref, st_ref, kv_ref, dq_zero, dkv_zero, dq_ref, dkv_ref,
    listed, low_ref, base_ref, bias_ref, w_buf, s_buf,
):
    tail = kv_ref[:, pl.ds(2 * TOK, 16), :].astype(F32)
    key_doc = tail[:, 0, :].astype(jnp.int32)
    key_base = tail[:, 1, :].astype(jnp.int32) * TOK
    base_ref[...] = key_base
    lane = lax.broadcasted_iota(jnp.int32, (GROUP, TOK), 1)
    key_place = key_base + lane
    query_doc = jnp.concatenate([st_ref[i, pl.ds(16, 1), :] for i in range(QS)], axis=0)
    query_doc = query_doc.astype(jnp.int32)
    query_place = jnp.concatenate([st_ref[i, pl.ds(17, 1), :] for i in range(QS)], axis=0)
    query_place = query_place.astype(jnp.int32)
    low = jnp.full((QS, TOK), FAR, jnp.int32)
    for d in range(DOCS):
        first = jnp.where(key_doc == d, key_place, FAR)
        first = jnp.min(jnp.min(first, axis=0, keepdims=True), axis=1, keepdims=True)
        low = jnp.where(query_doc == d, first, low)
    low_ref[pl.ds(0, QS), :] = low
    low_ref[pl.ds(QS, QS), :] = query_place
    key_row = lax.broadcasted_iota(jnp.int32, (GROUP, TOK), 0)
    count = jnp.int32(0)
    for i in range(QS):
        top = jnp.max(query_place[i : i + 1], axis=1, keepdims=True)
        least = jnp.min(low[i : i + 1], axis=1, keepdims=True)
        active = (key_base <= top) & (key_base + (TOK - 1) >= least)
        for part in range(2):
            bits = jnp.where(
                active & (key_row // 16 == part), jnp.left_shift(1, lax.rem(key_row, 16)), 0
            )
            word = jnp.max(jnp.sum(bits, axis=0, keepdims=True))

            def note(j, count, i=i, part=part, word=word):
                listed[count] = i * 64 + (part * 16 + j) * 2 + 1
                return count + (lax.shift_right_logical(word, j) & 1)

            for j in range(16):
                count = note(j, count)
        last = listed[jnp.maximum(count - 1, 0)]
        listed[count] = last & -2
        count = count + (count & 1)

    sublane = lax.broadcasted_iota(jnp.int32, (TOK, TOK), 0)
    score_scale = HD ** (-0.5) * LOG2E
    nt = (((1,), (1,)), ((), ()))


    w_buf[...] = jnp.zeros_like(w_buf)
    s_buf[...] = jnp.zeros_like(s_buf)

    def late(i, k0, k1):
        kk = jnp.concatenate([kv_ref[k0, pl.ds(0, TOK), :], kv_ref[k1, pl.ds(0, TOK), :]], axis=0)
        kt = kk.T

        stack_g = jnp.concatenate([g_ref[i, :, pl.ds(h * HD, HD)] for h in range(HEADS)], axis=0)
        stack_q = jnp.concatenate([q_ref[i, :, pl.ds(h * HD, HD)] for h in range(HEADS)], axis=0)

        dv = jnp.dot(w_buf[...], stack_g, preferred_element_type=F32)
        dk = jnp.dot(s_buf[...], stack_q, preferred_element_type=F32)

        dkv_ref[k0, pl.ds(0, TOK), :] += dk[:TOK]
        dkv_ref[k0, pl.ds(TOK, TOK), :] += dv[:TOK]
        dkv_ref[k1, pl.ds(0, TOK), :] += dk[TOK:]
        dkv_ref[k1, pl.ds(TOK, TOK), :] += dv[TOK:]

        dq_ref[i] += jnp.dot(kt, s_buf[...], preferred_element_type=F32)

    def over_pairs(pair, before):
        late(*before)
        one, two = listed[2 * pair], listed[2 * pair + 1]
        i = one // 64
        k0 = lax.rem(one // 2, GROUP)
        k1 = lax.rem(two // 2, GROUP)
        lo, hi = low_ref[pl.ds(i, 1), :], low_ref[pl.ds(QS + i, 1), :]
        b0, b1 = base_ref[pl.ds(k0, 1), :], base_ref[pl.ds(k1, 1), :]
        hi1 = jnp.where((two & 1) == 1, hi - b1, -1)
        bias_ref[pl.ds(0, TOK), :] = jnp.where(
            (sublane >= lo - b0) & (sublane <= hi - b0), 0.0, -1e30
        )
        bias_ref[pl.ds(TOK, TOK), :] = jnp.where(
            (sublane >= lo - b1) & (sublane <= hi1), 0.0, -1e30
        )
        kk = jnp.concatenate([kv_ref[k0, pl.ds(0, TOK), :], kv_ref[k1, pl.ds(0, TOK), :]], axis=0)
        vv = jnp.concatenate(
            [kv_ref[k0, pl.ds(TOK, TOK), :], kv_ref[k1, pl.ds(TOK, TOK), :]], axis=0
        )

        def heads(ref, hp):
            a = ref[i, :, pl.ds(2 * hp * HD, HD)]
            b = ref[i, :, pl.ds((2 * hp + 1) * HD, HD)]
            return jnp.concatenate([a, b], axis=0)

        def rows(first, hp):
            a = st_ref[i, pl.ds(first + 2 * hp, 1), :]
            b = st_ref[i, pl.ds(first + 2 * hp + 1, 1), :]
            return jnp.concatenate([a, b], axis=1)

        for hp in range(HEADS // 2):
            cols = pl.ds(2 * hp * HD, 2 * HD)
            hs = range(2 * hp, 2 * hp + 2)
            qh = jnp.concatenate([q_ref[i, :, pl.ds(h * HD, HD)] for h in hs], axis=0)
            gh = jnp.concatenate([g_ref[i, :, pl.ds(h * HD, HD)] for h in hs], axis=0)
            lse = jnp.concatenate([st_ref[i, pl.ds(h, 1), :] for h in hs], axis=1)
            delta = jnp.concatenate([st_ref[i, pl.ds(HEADS + h, 1), :] for h in hs], axis=1)
            scores = lax.dot_general(kk, qh, nt, preferred_element_type=F32)
            bias = bias_ref[...]
            bias = jnp.concatenate([bias] * 2, axis=1)
            weights = jnp.exp2(scores * score_scale + (bias - lse * LOG2E))
            w_buf[:, cols] = weights.astype(BF16)
            grads = lax.dot_general(vv, gh, nt, preferred_element_type=F32)
            s_buf[:, cols] = (weights * (grads - delta)).astype(BF16)
        return i, k0, k1

    start = (jnp.int32(0),) * 3
    late(*lax.fori_loop(0, count // 2, over_pairs, start))


def reduce_kernel(
    dq_ref, dkv_ref,
    dq_out, dk_out, dv_out,
    out1, in1, out2, in2, out3, in3, part1, near, sibq, farq_out, farq_in,
    s1, r1, s2, r2, s3, r3, sq, rq,
):
    at = Place()
    score_scale = HD ** (-0.5)
    sends = []

    def go(copy):
        copy.start()
        sends.append(copy)

    at.greet()
    qslot = at.zl * 2 + at.c
    sib_far = (1 - at.zl) * 2 + 1 - at.c
    sib_own = at.zl * 2 + 1 - at.c
    my_far = (1 - at.zl) * 2 + at.c
    CH = HD // 4

    def far_piece(n):
        rows = pl.ds(n * CH, CH)
        return remote(dq_ref.at[sib_far, rows], near.at[rows], sq.at[n], rq.at[n], at.sib)

    def far_send(n):
        rows = pl.ds(n * CH, CH)
        return remote(farq_out.at[rows], farq_in.at[rows], sq.at[4 + n], rq.at[4 + n], at.zq)

    own_piece = remote(dq_ref.at[sib_own], sibq, sq.at[8], rq.at[8], at.sib)
    for n in range(4):
        go(far_piece(n))
    go(own_piece)

    order = (2, 1, -1, 0)
    K, V = pl.ds(0, HD), pl.ds(HD, HD)

    def hop1(w, j, t):
        ahead = 1 if t % 2 == 0 else -1
        n = (w * 4 + j) * 6 + t
        return remote(
            out1.at[n], in1.at[n], s1.at[n], r1.at[n], at.nbr(w, 0, ahead)
        )

    def hop2(w, t):
        ahead = 1 if t % 2 == 0 else -1
        n = w * 6 + t
        return remote(out2.at[n], in2.at[n], s2.at[n], r2.at[n], at.nbr(w, ahead, 0))

    def first(w, j, t):
        dp = order[j]
        where = (2, 2, 1, -1)[t]
        rows = (K, V, V, K)[t]
        out1[(w * 4 + j) * 6 + t] = dkv_ref[at.slot(w, dp, where), rows, :].astype(BF16)
        go(hop1(w, j, t))

    def enter(j):
        for t in (0, 1, 2, 3):
            for w in (1, 0):
                first(w, j, t)

    def merge(j):
        for t, where, rows in ((4, 1, K), (5, -1, V)):
            for w in (1, 0):
                base = (w * 4 + j) * 6
                hop1(w, j, t - 4).wait_recv()
                own = dkv_ref[at.slot(w, order[j], where), rows, :]
                out1[base + t] = (own + in1[base + t - 4].astype(F32)).astype(BF16)
                go(hop1(w, j, t))

    def far(n):
        rows = pl.ds(n * CH, CH)
        far_piece(n).wait_recv()
        farq_out[rows, :] = (dq_ref[my_far, rows, :] + near[rows, :]).astype(BF16)
        go(far_send(n))

    def settle(w, j):
        base = (w * 4 + j) * 6
        for t in (2, 3, 4, 5):
            hop1(w, j, t).wait_recv()
        own = dkv_ref[at.slot(w, order[j], 0)]
        dk = own[:HD] + in1[base + 3].astype(F32) + in1[base + 4].astype(F32)
        dv = own[HD:] + in1[base + 2].astype(F32) + in1[base + 5].astype(F32)
        return dk, dv

    def second(w, t, value):
        out2[w * 6 + t] = value.astype(BF16)
        go(hop2(w, t))

    def total(w):
        dk, dv = settle(w, 3)
        for t in (2, 3, 4, 5):
            hop2(w, t).wait_recv()
        base = w * 6
        dk = dk + in2[base + 3].astype(F32) + in2[base + 4].astype(F32)
        dv = dv + in2[base + 2].astype(F32) + in2[base + 5].astype(F32)
        return dk, dv

    enter(0)
    enter(1)
    for n in range(4):
        far(n)
    merge(0)
    enter(2)
    merge(1)
    enter(3)
    for w in (1, 0):
        dk, dv = settle(w, 0)
        second(w, 0, dk)
        second(w, 1, dv)
    merge(2)
    for w in (1, 0):
        dk, dv = settle(w, 1)
        part1[w, 0] = dk
        second(w, 2, dv)
    merge(3)
    for w in (1, 0):
        dk, dv = settle(w, 2)
        part1[w, 1] = dv
        second(w, 3, dk)
    for w in (1, 0):
        hop2(w, 0).wait_recv()
        second(w, 4, part1[w, 0] + in2[w * 6].astype(F32))
        hop2(w, 1).wait_recv()
        second(w, 5, part1[w, 1] + in2[w * 6 + 1].astype(F32))

    across = [remote(out3.at[n], in3.at[n], s3.at[n], r3.at[n], at.zk) for n in range(2)]
    dk, dv = total(1)
    out3[0] = dk.astype(BF16)
    go(across[0])
    out3[1] = dv.astype(BF16)
    go(across[1])
    own_piece.wait_recv()
    for n in range(4):
        far_send(n).wait_recv()
    for h in range(HEADS):
        cols = pl.ds(h * HD, HD)
        value = dq_ref[qslot, :, cols] + sibq[:, cols] + farq_in[:, cols].astype(F32)
        dq_out[:, cols] = (value * score_scale).T.astype(BF16)
    dk, dv = total(0)
    across[0].wait_recv()
    dk_out[...] = ((dk + in3[0].astype(F32)) * score_scale).astype(BF16)
    across[1].wait_recv()
    dv_out[...] = (dv + in3[1].astype(F32)).astype(BF16)
    for copy in sends:
        copy.wait_send()


def store_kernel(dq_in, dk_in, dv_in, dq_out, dk_out, dv_out, sem):
    copies = [
        pltpu.make_async_copy(dq_in, dq_out, sem.at[0]),
        pltpu.make_async_copy(dk_in, dk_out, sem.at[1]),
        pltpu.make_async_copy(dv_in, dv_out, sem.at[2]),
    ]
    for copy in copies:
        copy.start()
    for copy in copies:
        copy.wait()


HB = pl.BlockSpec(memory_space=pltpu.HBM)
VM = pl.BlockSpec(memory_space=pltpu.VMEM)
DMA = pltpu.SemaphoreType.DMA


def gather(queries, key_rows, value_rows, forward_out, out_grad, logsumexp, position, segment):
    wide = HEADS * HD
    args = (
        queries, key_rows, value_rows, forward_out, out_grad,
        logsumexp, position.reshape(1, TOK), segment.reshape(1, TOK),
    )
    return pl.pallas_call(
        gather_kernel,
        out_shape=(
            pltpu.VMEM((QS, TOK, wide), BF16),
            pltpu.VMEM((QS, TOK, wide), BF16),
            pltpu.VMEM((QS, STR, TOK), F32),
            pltpu.VMEM((GROUP, KVR, HD), BF16),
            pltpu.VMEM((QS, HD, wide), F32),
            pltpu.VMEM((GROUP, 2 * HD, HD), F32),
        ),
        in_specs=[HB] * 8,
        out_specs=(VM,) * 6,
        scratch_shapes=[
            pltpu.VMEM((TOK, wide), BF16),
            pltpu.VMEM((HEADS, TOK), F32),
            pltpu.VMEM((1, TOK), jnp.int32),
            pltpu.VMEM((1, TOK), jnp.int32),
            DMA((8,)),
            DMA((41,)),
            DMA((41,)),
            DMA((15,)),
            DMA((15,)),
        ],
        compiler_params=pltpu.CompilerParams(
            collective_id=0, has_side_effects=True, vmem_limit_bytes=8 << 20
        ),
        name="gather_rows",
    )(*[pltpu.with_memory_space_constraint(a, pltpu.HBM) for a in args])


def grads(q_all, g_all, st_all, kv_all, dq_zero, dkv_zero):
    wide = HEADS * HD
    return pl.pallas_call(
        grads_kernel,
        out_shape=(
            pltpu.VMEM((QS, HD, wide), F32),
            pltpu.VMEM((GROUP, 2 * HD, HD), F32),
        ),
        in_specs=[VM] * 6,
        out_specs=(VM,) * 2,
        input_output_aliases={4: 0, 5: 1},
        scratch_shapes=[
            pltpu.SMEM((QS * GROUP + 16,), jnp.int32),
            pltpu.VMEM((2 * QS, TOK), jnp.int32),
            pltpu.VMEM((GROUP, TOK), jnp.int32),
            pltpu.VMEM((2 * TOK, TOK), F32),
            pltpu.VMEM((2 * TOK, wide), BF16),
            pltpu.VMEM((2 * TOK, wide), BF16),
        ],
        compiler_params=pltpu.CompilerParams(vmem_limit_bytes=24 << 20),
        name="tile_grads",
    )(q_all, g_all, st_all, kv_all, dq_zero, dkv_zero)


def reduce(dq_all, dkv_all):
    wide = HEADS * HD
    return pl.pallas_call(
        reduce_kernel,
        out_shape=(
            pltpu.VMEM((TOK, wide), BF16),
            pltpu.VMEM((TOK, HD), BF16),
            pltpu.VMEM((TOK, HD), BF16),
        ),
        in_specs=[VM] * 2,
        out_specs=(VM,) * 3,
        scratch_shapes=[
            pltpu.VMEM((48, HD, HD), BF16),
            pltpu.VMEM((48, HD, HD), BF16),
            pltpu.VMEM((12, HD, HD), BF16),
            pltpu.VMEM((12, HD, HD), BF16),
            pltpu.VMEM((2, HD, HD), BF16),
            pltpu.VMEM((2, HD, HD), BF16),
            pltpu.VMEM((2, 2, HD, HD), F32),
            pltpu.VMEM((HD, wide), F32),
            pltpu.VMEM((HD, wide), F32),
            pltpu.VMEM((HD, wide), BF16),
            pltpu.VMEM((HD, wide), BF16),
            DMA((48,)), DMA((48,)), DMA((12,)), DMA((12,)), DMA((2,)), DMA((2,)), DMA((9,)), DMA((9,)),
        ],
        compiler_params=pltpu.CompilerParams(
            collective_id=1, has_side_effects=True, vmem_limit_bytes=24 << 20
        ),
        name="reduce_grads",
    )(dq_all, dkv_all)


def store(dq, dk, dv):
    return pl.pallas_call(
        store_kernel,
        out_shape=tuple(pltpu.HBM(a.shape, BF16) for a in (dq, dk, dv)),
        in_specs=[VM] * 3,
        out_specs=(HB,) * 3,
        scratch_shapes=[DMA((3,))],
        name="store_grads",
    )(*[pltpu.with_memory_space_constraint(a, pltpu.VMEM) for a in (dq, dk, dv)])


def body(*args):
    return store(*reduce(*grads(*gather(*args))))


def solution(mesh):
    rows = P(("pb", "ka"), None)
    flat = P(("pb", "ka"))
    placed = (rows,) * 5 + (P(None, ("pb", "ka")), flat, flat)
    return jax.shard_map(
        body, mesh=mesh, in_specs=placed, out_specs=(rows,) * 3, check_vma=False
    )
```

```python
import functools

import jax
import jax.numpy as jnp
from jax import lax
from jax.experimental import pallas as pl
from jax.experimental.pallas import tpu as pltpu
from jax.sharding import PartitionSpec as P

MESH = pl.DeviceIdType.MESH
F32 = jnp.float32
BF16 = jnp.bfloat16
SIDE = 4
HEADS = 8
HD = 128
TOK = 128
GROUP = 2 * SIDE * SIDE
QS = 4
KVR = 272
STR = 24
DOCS = 8
FAR = 1 << 20
LOG2E = 1.4426950408889634

FIRST_OUT = (
    ("z", 0, 0, 0, 0), ("z", 0, 0, 0, 1), ("t", 0, 0, 0, 0), ("t", 0, 0, 1, 1),
    ("d", 0, 0, 0, 0), ("d", 0, 0, 1, 1), ("d", 0, 0, 0, 1), ("d", 0, 0, 1, 0),
    ("s", 0, 0, 0, 0), ("s", 0, 0, 1, 1), ("s", 0, 0, 0, 1), ("s", 0, 0, 1, 0),
)
THEN_OUT = (
    ("t", 1, 0, 0, 0), ("s", 1, 0, 1, 0), ("d", 1, 0, 0, 0), ("d", 1, 0, 1, 0),
    ("g", 0, 0, 1, 1), ("d", 1, 0, 1, 1), ("d", 1, 0, 0, 1), ("s", 1, 0, 0, 0),
    ("t", 1, 0, 1, 1), ("r", 0, 0, 0, 0), ("s", 1, 0, 0, 1), ("d", 0, 2, 0, 0),
    ("s", 1, 0, 1, 1), ("d", 1, 2, 0, 0), ("d", 1, 2, 1, 0), ("d", 0, 2, 0, 1),
    ("g", 1, 0, 0, 0), ("d", 0, 2, 1, 1), ("g", 1, 0, 1, 1), ("d", 0, 1, 0, 0),
    ("d", 1, 1, 0, 0), ("d", 0, 2, 1, 0), ("d", 1, 1, 1, 0), ("r", 1, 0, 0, 0),
    ("d", 0, 3, 0, 0), ("d", 1, 3, 0, 0), ("d", 0, 1, 1, 1), ("d", 1, 1, 1, 1),
    ("g", 0, 0, 0, 0), ("d", 1, 1, 0, 1), ("d", 0, 3, 1, 1), ("d", 1, 2, 1, 1),
    ("g", 0, 2, 0, 0), ("g", 1, 2, 0, 0), ("d", 0, 1, 1, 0), ("d", 1, 3, 1, 1),
    ("d", 0, 1, 0, 1), ("d", 1, 2, 0, 1), ("g", 0, 2, 1, 1), ("r", 2, 0, 0, 0),
    ("d", 1, 3, 1, 0), ("g", 0, 1, 0, 0), ("g", 1, 1, 0, 0), ("d", 0, 3, 1, 0),
    ("g", 0, 3, 0, 0), ("g", 1, 1, 1, 1), ("g", 1, 3, 0, 0), ("g", 0, 1, 1, 1),
    ("d", 0, 3, 0, 1), ("g", 1, 2, 1, 1), ("d", 1, 3, 0, 1), ("g", 0, 3, 1, 1),
    ("g", 1, 3, 1, 1), ("r", 3, 0, 0, 0), ("r", 4, 0, 0, 0),
)
TERMS_OUT = (
    ("h", 1, 1, 1), ("h", 1, 1, 0), ("h", 0, 1, 1), ("h", 0, 1, 0), ("h", 1, 1, 3),
    ("h", 1, 1, 2), ("h", 0, 1, 2), ("h", 0, 1, 3), ("h", 1, 0, 0), ("h", 1, 0, 1),
    ("h", 0, 0, 0), ("h", 0, 0, 3), ("h", 1, 0, 2), ("h", 1, 0, 3), ("h", 0, 0, 1),
    ("h", 0, 0, 2), ("h", 1, 2, 1), ("h", 1, 2, 0), ("h", 0, 2, 0), ("h", 0, 2, 1),
    ("h", 1, 1, 5), ("h", 1, 1, 4), ("h", 0, 1, 5), ("h", 0, 1, 4), ("h", 1, 2, 2),
    ("h", 1, 2, 3), ("h", 0, 2, 2), ("h", 0, 2, 3), ("h", 1, 0, 5), ("h", 1, 0, 4),
    ("h", 0, 0, 4), ("h", 0, 3, 1), ("h", 0, 0, 5), ("h", 1, 3, 0), ("h", 1, 3, 1),
    ("h", 0, 3, 0), ("h", 1, 2, 5), ("h", 1, 2, 4), ("h", 0, 2, 5), ("h", 0, 2, 4),
    ("n", 1, 1, 0), ("n", 0, 1, 0), ("h", 1, 3, 3), ("h", 0, 3, 3), ("t", 1, 0, 1),
    ("t", 1, 0, 0), ("h", 1, 3, 2), ("h", 1, 3, 5), ("h", 1, 3, 4), ("n", 1, 2, 0),
    ("t", 0, 0, 1), ("t", 0, 0, 0), ("h", 0, 3, 4), ("h", 0, 3, 2), ("n", 0, 2, 0),
    ("h", 0, 3, 5), ("x", 1, 0, 0), ("x", 1, 0, 1),
)


class Place:
    def __init__(self):
        pb, ka = lax.axis_index("pb"), lax.axis_index("ka")
        self.c, self.zh = lax.rem(pb, 2), pb // 2
        self.zl, u = lax.rem(ka, 2), ka // 2
        self.x, self.y = u // SIDE, lax.rem(u, SIDE)
        self.z = self.zh * 2 + self.zl
        self.half = (1 - self.zl, self.zl)
        self.sib = self.dev(self.x, self.y, self.z, 1 - self.c)
        self.zq = self.dev(self.x, self.y, self.zh * 2 + 1 - self.zl, self.c)
        self.zk = self.dev(self.x, self.y, lax.rem(self.z + 3 + 2 * self.zl, SIDE), self.c)

    def dev(self, x, y, z, c):
        return {"pb": (z // 2) * 2 + c, "ka": (x * SIDE + y) * 2 + lax.rem(z, 2)}

    def moved(self, w, dp, ds):
        hw = self.half[w]
        x = lax.rem(self.x + SIDE + dp * (1 - hw) + ds * hw, SIDE)
        y = lax.rem(self.y + SIDE + dp * hw + ds * (1 - hw), SIDE)
        return x, y

    def nbr(self, w, dp, ds):
        x, y = self.moved(w, dp, ds)
        return self.dev(x, y, self.z, self.c)

    def slot(self, w, dp, ds):
        x, y = self.moved(w, dp, ds)
        return (x * SIDE + y) * 2 + self.half[w]

    def greet(self):
        partners = [
            self.sib,
            self.zq,
            self.zk,
            self.nbr(0, 1, 0),
            self.nbr(0, -1, 0),
            self.nbr(0, 0, 1),
            self.nbr(0, 0, -1),
            self.nbr(0, 2, 0),
            self.nbr(0, 0, 2),
        ]
        barrier = pltpu.get_barrier_semaphore()
        for partner in partners:
            pl.semaphore_signal(barrier, inc=1, device_id=partner, device_id_type=MESH)
        pl.semaphore_wait(barrier, len(partners))


def remote(src, dst, send_sem, recv_sem, device):
    return pltpu.make_async_remote_copy(
        src_ref=src,
        dst_ref=dst,
        send_sem=send_sem,
        recv_sem=recv_sem,
        device_id=device,
        device_id_type=MESH,
    )


def gather_kernel(
    q_in, k_in, v_in, o_in, g_in, lse_in, pos_in, seg_in,
    q_all, g_all, st_all, kv_all, dq_zero, dkv_zero,
    o_buf, lse_buf, pos_buf, seg_buf, loc, ksend, krecv, qsend, qrecv,
):
    at = Place()
    slot = at.slot(0, 0, 0)
    qslot = at.zl * 2 + at.c
    local = [
        pltpu.make_async_copy(k_in, kv_all.at[slot, pl.ds(0, TOK)], loc.at[0]),
        pltpu.make_async_copy(v_in, kv_all.at[slot, pl.ds(TOK, TOK)], loc.at[1]),
        pltpu.make_async_copy(q_in, q_all.at[qslot], loc.at[2]),
        pltpu.make_async_copy(g_in, g_all.at[qslot], loc.at[3]),
        pltpu.make_async_copy(o_in, o_buf, loc.at[4]),
        pltpu.make_async_copy(lse_in, lse_buf, loc.at[5]),
        pltpu.make_async_copy(pos_in, pos_buf, loc.at[6]),
        pltpu.make_async_copy(seg_in, seg_buf, loc.at[7]),
    ]
    for copy in (local[6], local[7], *local[:6]):
        copy.start()
    at.greet()
    local[6].wait()
    local[7].wait()
    seg = seg_buf[...].astype(F32)
    pos = pos_buf[...].astype(F32)
    row = lax.broadcasted_iota(jnp.int32, (16, TOK), 0)
    block_number = (pos_buf[...] // TOK).astype(F32)
    kv_all[slot, pl.ds(2 * TOK, 16), :] = jnp.where(row == 0, seg, block_number).astype(BF16)
    sends, arrived = [], set()
    numbers = {m: n for n, m in enumerate(m for m in FIRST_OUT + THEN_OUT if m[0] != "r")}
    columns = (0, -1, 1, 2)

    def route(m):
        kind, w, j, d, h = m
        way = 1 - 2 * d
        if kind == "z":
            return slot, at.slot(1, 0, 0), at.zk
        if kind == "s":
            return at.slot(w, 0, 0), at.slot(w, -way, 0), at.nbr(w, way, 0)
        if kind == "t":
            return at.slot(w, 0, 0), at.slot(w, 2, 0), at.nbr(w, 2, 0)
        dp = columns[j]
        if kind == "d":
            return at.slot(w, dp, 0), at.slot(w, dp, -way), at.nbr(w, 0, way)
        return at.slot(w, dp, -way), at.slot(w, dp, 2), at.nbr(w, 0, way)

    def needs(m):
        kind, w, j, d, h = m
        if kind == "g":
            return ("d", w, j, h, h)
        if kind == "d" and j > 0:
            return (None, ("s", w, 0, 0, h), ("s", w, 0, 1, h), ("t", w, 0, h, h))[j]
        return ("z", 0, 0, 0, h) if w == 1 else None

    def kv_copy(m, where, device):
        part = kv_all.at[where, pl.ds(0, TOK) if m[4] == 0 else pl.ds(TOK, KVR - TOK)]
        return remote(part, part, ksend.at[numbers[m]], krecv.at[numbers[m]], device)

    def go(copy):
        copy.start()
        sends.append(copy)

    def arrive(m):
        if m not in arrived:
            arrived.add(m)
            _, where, device = route(m)
            kv_copy(m, where, device).wait_recv()

    def send(m):
        if needs(m):
            arrive(needs(m))
        where, _, device = route(m)
        go(kv_copy(m, where, device))

    def piece(who, n):
        if n < 4:
            ref = q_all if n < 2 else g_all
            return ref.at[who, pl.ds((n % 2) * (TOK // 2), TOK // 2)]
        return st_all.at[who]

    def q_copy(kind, n, who, device):
        part = piece(who, n)
        return remote(part, part, qsend.at[5 * kind + n], qrecv.at[5 * kind + n], device)

    local[0].wait()
    local[1].wait()
    for m in FIRST_OUT:
        send(m)
    local[2].wait()
    for n in (0, 1):
        go(q_copy(0, n, qslot, at.zq))
    local[3].wait()
    for n in (2, 3):
        go(q_copy(0, n, qslot, at.zq))
    for n in range(4):
        go(q_copy(1, n, qslot, at.sib))

    local[4].wait()
    local[5].wait()
    st_all[qslot, pl.ds(0, HEADS), :] = lse_buf[...]
    for h in range(HEADS):
        cols = pl.ds(h * HD, HD)
        prod = g_all[qslot, :, cols].astype(F32) * o_buf[:, cols].astype(F32)
        st_all[qslot, pl.ds(HEADS + h, 1), :] = jnp.sum(prod.T, axis=0, keepdims=True)
    row = lax.broadcasted_iota(jnp.int32, (8, TOK), 0)
    st_all[qslot, pl.ds(16, 8), :] = jnp.where(row == 0, seg, pos)
    dq_zero[...] = jnp.zeros_like(dq_zero)
    dkv_zero[...] = jnp.zeros_like(dkv_zero)
    go(q_copy(0, 4, qslot, at.zq))
    go(q_copy(1, 4, qslot, at.sib))

    far = (1 - at.zl) * 2 + at.c
    for m in THEN_OUT:
        if m[0] == "r":
            q_copy(0, m[1], far, at.zq).wait_recv()
            go(q_copy(2, m[1], far, at.sib))
        else:
            send(m)
    for m in numbers:
        arrive(m)
    for n in range(5):
        q_copy(1, n, at.zl * 2 + 1 - at.c, at.sib).wait_recv()
        q_copy(2, n, (1 - at.zl) * 2 + 1 - at.c, at.sib).wait_recv()
    for copy in sends:
        copy.wait_send()


def grads_kernel(
    q_ref, g_ref, st_ref, kv_ref, dq_zero, dkv_zero, dq_ref, dkv_ref,
    listed, low_ref, base_ref, bias_ref, w_buf, s_buf,
):
    tail = kv_ref[:, pl.ds(2 * TOK, 16), :].astype(F32)
    key_doc = tail[:, 0, :].astype(jnp.int32)
    key_base = tail[:, 1, :].astype(jnp.int32) * TOK
    base_ref[...] = key_base
    lane = lax.broadcasted_iota(jnp.int32, (GROUP, TOK), 1)
    key_place = key_base + lane
    query_doc = jnp.concatenate([st_ref[i, pl.ds(16, 1), :] for i in range(QS)], axis=0)
    query_doc = query_doc.astype(jnp.int32)
    query_place = jnp.concatenate([st_ref[i, pl.ds(17, 1), :] for i in range(QS)], axis=0)
    query_place = query_place.astype(jnp.int32)
    low = jnp.full((QS, TOK), FAR, jnp.int32)
    for d in range(DOCS):
        first = jnp.where(key_doc == d, key_place, FAR)
        first = jnp.min(jnp.min(first, axis=0, keepdims=True), axis=1, keepdims=True)
        low = jnp.where(query_doc == d, first, low)
    low_ref[pl.ds(0, QS), :] = low
    low_ref[pl.ds(QS, QS), :] = query_place
    key_row = lax.broadcasted_iota(jnp.int32, (GROUP, TOK), 0)
    count = jnp.int32(0)
    for i in range(QS):
        top = jnp.max(query_place[i : i + 1], axis=1, keepdims=True)
        least = jnp.min(low[i : i + 1], axis=1, keepdims=True)
        active = (key_base <= top) & (key_base + (TOK - 1) >= least)
        for part in range(2):
            bits = jnp.where(
                active & (key_row // 16 == part), jnp.left_shift(1, lax.rem(key_row, 16)), 0
            )
            word = jnp.max(jnp.sum(bits, axis=0, keepdims=True))

            def note(j, count, i=i, part=part, word=word):
                listed[count] = i * 64 + (part * 16 + j) * 2 + 1
                return count + (lax.shift_right_logical(word, j) & 1)

            for j in range(16):
                count = note(j, count)
        last = listed[jnp.maximum(count - 1, 0)]
        listed[count] = last & -2
        count = count + (count & 1)

    sublane = lax.broadcasted_iota(jnp.int32, (TOK, TOK), 0)
    score_scale = HD ** (-0.5) * LOG2E
    nt = (((1,), (1,)), ((), ()))


    w_buf[...] = jnp.zeros_like(w_buf)
    s_buf[...] = jnp.zeros_like(s_buf)

    def late(i, k0, k1):
        kk = jnp.concatenate([kv_ref[k0, pl.ds(0, TOK), :], kv_ref[k1, pl.ds(0, TOK), :]], axis=0)
        kt = kk.T

        stack_g = jnp.concatenate([g_ref[i, :, pl.ds(h * HD, HD)] for h in range(HEADS)], axis=0)
        stack_q = jnp.concatenate([q_ref[i, :, pl.ds(h * HD, HD)] for h in range(HEADS)], axis=0)

        dv = jnp.dot(w_buf[...], stack_g, preferred_element_type=F32)
        dk = jnp.dot(s_buf[...], stack_q, preferred_element_type=F32)

        dkv_ref[k0, pl.ds(0, TOK), :] += dk[:TOK]
        dkv_ref[k0, pl.ds(TOK, TOK), :] += dv[:TOK]
        dkv_ref[k1, pl.ds(0, TOK), :] += dk[TOK:]
        dkv_ref[k1, pl.ds(TOK, TOK), :] += dv[TOK:]

        dq_ref[i] += jnp.dot(kt, s_buf[...], preferred_element_type=F32)

    def over_pairs(pair, before):
        late(*before)
        one, two = listed[2 * pair], listed[2 * pair + 1]
        i = one // 64
        k0 = lax.rem(one // 2, GROUP)
        k1 = lax.rem(two // 2, GROUP)
        lo, hi = low_ref[pl.ds(i, 1), :], low_ref[pl.ds(QS + i, 1), :]
        b0, b1 = base_ref[pl.ds(k0, 1), :], base_ref[pl.ds(k1, 1), :]
        hi1 = jnp.where((two & 1) == 1, hi - b1, -1)
        bias_ref[pl.ds(0, TOK), :] = jnp.where(
            (sublane >= lo - b0) & (sublane <= hi - b0), 0.0, -1e30
        )
        bias_ref[pl.ds(TOK, TOK), :] = jnp.where(
            (sublane >= lo - b1) & (sublane <= hi1), 0.0, -1e30
        )
        kk = jnp.concatenate([kv_ref[k0, pl.ds(0, TOK), :], kv_ref[k1, pl.ds(0, TOK), :]], axis=0)
        vv = jnp.concatenate(
            [kv_ref[k0, pl.ds(TOK, TOK), :], kv_ref[k1, pl.ds(TOK, TOK), :]], axis=0
        )

        def heads(ref, hp):
            a = ref[i, :, pl.ds(2 * hp * HD, HD)]
            b = ref[i, :, pl.ds((2 * hp + 1) * HD, HD)]
            return jnp.concatenate([a, b], axis=0)

        def rows(first, hp):
            a = st_ref[i, pl.ds(first + 2 * hp, 1), :]
            b = st_ref[i, pl.ds(first + 2 * hp + 1, 1), :]
            return jnp.concatenate([a, b], axis=1)

        for hp in range(HEADS // 2):
            cols = pl.ds(2 * hp * HD, 2 * HD)
            hs = range(2 * hp, 2 * hp + 2)
            qh = jnp.concatenate([q_ref[i, :, pl.ds(h * HD, HD)] for h in hs], axis=0)
            gh = jnp.concatenate([g_ref[i, :, pl.ds(h * HD, HD)] for h in hs], axis=0)
            lse = jnp.concatenate([st_ref[i, pl.ds(h, 1), :] for h in hs], axis=1)
            delta = jnp.concatenate([st_ref[i, pl.ds(HEADS + h, 1), :] for h in hs], axis=1)
            scores = lax.dot_general(kk, qh, nt, preferred_element_type=F32)
            bias = bias_ref[...]
            bias = jnp.concatenate([bias] * 2, axis=1)
            weights = jnp.exp2(scores * score_scale + (bias - lse * LOG2E))
            w_buf[:, cols] = weights.astype(BF16)
            grads = lax.dot_general(vv, gh, nt, preferred_element_type=F32)
            s_buf[:, cols] = (weights * (grads - delta)).astype(BF16)
        return i, k0, k1

    start = (jnp.int32(0),) * 3
    late(*lax.fori_loop(0, count // 2, over_pairs, start))


def reduce_kernel(
    dq_ref, dkv_ref,
    dq_out, dk_out, dv_out,
    out1, in1, out2, in2, out3, in3, near, sibq, farq_out, farq_in,
    s1, r1, s2, r2, s3, r3, sq, rq,
):
    at = Place()
    score_scale = HD ** (-0.5)
    sends = []

    def go(copy):
        copy.start()
        sends.append(copy)

    at.greet()
    qslot = at.zl * 2 + at.c
    sib_far = (1 - at.zl) * 2 + 1 - at.c
    sib_own = at.zl * 2 + 1 - at.c
    my_far = (1 - at.zl) * 2 + at.c
    CH = HD // 4

    def far_piece(n):
        rows = pl.ds(n * CH, CH)
        return remote(dq_ref.at[sib_far, rows], near.at[rows], sq.at[n], rq.at[n], at.sib)

    def far_send(n):
        rows = pl.ds(n * CH, CH)
        return remote(farq_out.at[rows], farq_in.at[rows], sq.at[4 + n], rq.at[4 + n], at.zq)

    own_piece = remote(dq_ref.at[sib_own], sibq, sq.at[8], rq.at[8], at.sib)
    for n in range(4):
        go(far_piece(n))
    go(own_piece)

    order = (2, 1, -1, 0)
    K, V = pl.ds(0, HD), pl.ds(HD, HD)

    def hop1(w, j, t):
        ahead = 1 if t % 2 == 0 else -1
        n = (w * 4 + j) * 6 + t
        return remote(out1.at[n], in1.at[n], s1.at[n], r1.at[n], at.nbr(w, 0, ahead))

    def first(w, j, t):
        where = (2, 2, 1, -1, 1, -1)[t]
        rows = (K, V, V, K, K, V)[t]
        value = dkv_ref[at.slot(w, order[j], where), rows, :]
        n = (w * 4 + j) * 6 + t
        if t >= 4:
            hop1(w, j, t - 4).wait_recv()
            value = value + in1[n - 4].astype(F32)
        out1[n] = value.astype(BF16)
        go(hop1(w, j, t))

    def settle(w, j):
        base = (w * 4 + j) * 6
        for t in (2, 3, 4, 5):
            hop1(w, j, t).wait_recv()
        own = dkv_ref[at.slot(w, order[j], 0)]
        dk = own[:HD] + in1[base + 3].astype(F32) + in1[base + 4].astype(F32)
        dv = own[HD:] + in1[base + 2].astype(F32) + in1[base + 5].astype(F32)
        return dk, dv

    def whole(w, j):
        n = w * 3 + j
        return remote(out2.at[n], in2.at[n], s2.at[4 + n], r2.at[4 + n], at.nbr(w, order[j], 0))

    def side(w, t):
        n = w * 3
        return remote(
            out2.at[n, t], in2.at[n, t], s2.at[2 * w + t], r2.at[2 * w + t], at.nbr(w, 2, 0)
        )

    def total(w):
        dk, dv = settle(w, 3)
        for t in (0, 1):
            side(w, t).wait_recv()
        for j in (1, 2):
            whole(w, j).wait_recv()
        for j in (0, 1, 2):
            dk = dk + in2[w * 3 + j, 0].astype(F32)
            dv = dv + in2[w * 3 + j, 1].astype(F32)
        return dk, dv

    def far(n):
        rows = pl.ds(n * CH, CH)
        far_piece(n).wait_recv()
        farq_out[rows, :] = (dq_ref[my_far, rows, :] + near[rows, :]).astype(BF16)
        go(far_send(n))

    across = [remote(out3.at[n], in3.at[n], s3.at[n], r3.at[n], at.zk) for n in range(2)]
    known = {}

    def sums(w, j):
        if (w, j) not in known:
            known[w, j] = total(w) if j == 3 else settle(w, j)
        return known[w, j]

    for n, (kind, w, j, t) in enumerate(TERMS_OUT):
        if n in (16, 18, 20, 22):
            far((n - 16) // 2)
        if kind == "h":
            first(w, j, t)
        elif kind == "t":
            out2[w * 3, t] = sums(w, 0)[t].astype(BF16)
            go(side(w, t))
        elif kind == "n":
            dk, dv = sums(w, j)
            out2[w * 3 + j, 0] = dk.astype(BF16)
            out2[w * 3 + j, 1] = dv.astype(BF16)
            go(whole(w, j))
        else:
            out3[t] = sums(1, 3)[t].astype(BF16)
            go(across[t])
    own_piece.wait_recv()
    for n in range(4):
        far_send(n).wait_recv()
    for h in range(HEADS):
        cols = pl.ds(h * HD, HD)
        value = dq_ref[qslot, :, cols] + sibq[:, cols] + farq_in[:, cols].astype(F32)
        dq_out[:, cols] = (value * score_scale).T.astype(BF16)
    dk, dv = total(0)
    across[0].wait_recv()
    dk_out[...] = ((dk + in3[0].astype(F32)) * score_scale).astype(BF16)
    across[1].wait_recv()
    dv_out[...] = (dv + in3[1].astype(F32)).astype(BF16)
    for copy in sends:
        copy.wait_send()


def store_kernel(dq_in, dk_in, dv_in, dq_out, dk_out, dv_out, sem):
    copies = [
        pltpu.make_async_copy(dq_in, dq_out, sem.at[0]),
        pltpu.make_async_copy(dk_in, dk_out, sem.at[1]),
        pltpu.make_async_copy(dv_in, dv_out, sem.at[2]),
    ]
    for copy in copies:
        copy.start()
    for copy in copies:
        copy.wait()


HB = pl.BlockSpec(memory_space=pltpu.HBM)
VM = pl.BlockSpec(memory_space=pltpu.VMEM)
DMA = pltpu.SemaphoreType.DMA


def gather(queries, key_rows, value_rows, forward_out, out_grad, logsumexp, position, segment):
    wide = HEADS * HD
    args = (
        queries, key_rows, value_rows, forward_out, out_grad,
        logsumexp, position.reshape(1, TOK), segment.reshape(1, TOK),
    )
    return pl.pallas_call(
        gather_kernel,
        out_shape=(
            pltpu.VMEM((QS, TOK, wide), BF16),
            pltpu.VMEM((QS, TOK, wide), BF16),
            pltpu.VMEM((QS, STR, TOK), F32),
            pltpu.VMEM((GROUP, KVR, HD), BF16),
            pltpu.VMEM((QS, HD, wide), F32),
            pltpu.VMEM((GROUP, 2 * HD, HD), F32),
        ),
        in_specs=[HB] * 8,
        out_specs=(VM,) * 6,
        scratch_shapes=[
            pltpu.VMEM((TOK, wide), BF16),
            pltpu.VMEM((HEADS, TOK), F32),
            pltpu.VMEM((1, TOK), jnp.int32),
            pltpu.VMEM((1, TOK), jnp.int32),
            DMA((8,)),
            DMA((62,)),
            DMA((62,)),
            DMA((15,)),
            DMA((15,)),
        ],
        compiler_params=pltpu.CompilerParams(
            collective_id=0, has_side_effects=True, vmem_limit_bytes=8 << 20
        ),
        name="gather_rows",
    )(*[pltpu.with_memory_space_constraint(a, pltpu.HBM) for a in args])


def grads(q_all, g_all, st_all, kv_all, dq_zero, dkv_zero):
    wide = HEADS * HD
    return pl.pallas_call(
        grads_kernel,
        out_shape=(
            pltpu.VMEM((QS, HD, wide), F32),
            pltpu.VMEM((GROUP, 2 * HD, HD), F32),
        ),
        in_specs=[VM] * 6,
        out_specs=(VM,) * 2,
        input_output_aliases={4: 0, 5: 1},
        scratch_shapes=[
            pltpu.SMEM((QS * GROUP + 16,), jnp.int32),
            pltpu.VMEM((2 * QS, TOK), jnp.int32),
            pltpu.VMEM((GROUP, TOK), jnp.int32),
            pltpu.VMEM((2 * TOK, TOK), F32),
            pltpu.VMEM((2 * TOK, wide), BF16),
            pltpu.VMEM((2 * TOK, wide), BF16),
        ],
        compiler_params=pltpu.CompilerParams(vmem_limit_bytes=24 << 20),
        name="tile_grads",
    )(q_all, g_all, st_all, kv_all, dq_zero, dkv_zero)


def reduce(dq_all, dkv_all):
    wide = HEADS * HD
    return pl.pallas_call(
        reduce_kernel,
        out_shape=(
            pltpu.VMEM((TOK, wide), BF16),
            pltpu.VMEM((TOK, HD), BF16),
            pltpu.VMEM((TOK, HD), BF16),
        ),
        in_specs=[VM] * 2,
        out_specs=(VM,) * 3,
        scratch_shapes=[
            pltpu.VMEM((48, HD, HD), BF16),
            pltpu.VMEM((48, HD, HD), BF16),
            pltpu.VMEM((6, 2, HD, HD), BF16),
            pltpu.VMEM((6, 2, HD, HD), BF16),
            pltpu.VMEM((2, HD, HD), BF16),
            pltpu.VMEM((2, HD, HD), BF16),
            pltpu.VMEM((HD, wide), F32),
            pltpu.VMEM((HD, wide), F32),
            pltpu.VMEM((HD, wide), BF16),
            pltpu.VMEM((HD, wide), BF16),
            DMA((48,)), DMA((48,)), DMA((10,)), DMA((10,)), DMA((2,)), DMA((2,)), DMA((9,)), DMA((9,)),
        ],
        compiler_params=pltpu.CompilerParams(
            collective_id=1, has_side_effects=True, vmem_limit_bytes=24 << 20
        ),
        name="reduce_grads",
    )(dq_all, dkv_all)


def store(dq, dk, dv):
    return pl.pallas_call(
        store_kernel,
        out_shape=tuple(pltpu.HBM(a.shape, BF16) for a in (dq, dk, dv)),
        in_specs=[VM] * 3,
        out_specs=(HB,) * 3,
        scratch_shapes=[DMA((3,))],
        name="store_grads",
    )(*[pltpu.with_memory_space_constraint(a, pltpu.VMEM) for a in (dq, dk, dv)])


def body(*args):
    return store(*reduce(*grads(*gather(*args))))


def solution(mesh):
    rows = P(("pb", "ka"), None)
    flat = P(("pb", "ka"))
    placed = (rows,) * 5 + (P(None, ("pb", "ka")), flat, flat)
    return jax.shard_map(
        body, mesh=mesh, in_specs=placed, out_specs=(rows,) * 3, check_vma=False
    )
```

```python
import functools

import jax
import jax.numpy as jnp
from jax import lax
from jax.experimental import pallas as pl
from jax.experimental.pallas import tpu as pltpu
from jax.sharding import PartitionSpec as P

MESH = pl.DeviceIdType.MESH
F32 = jnp.float32
BF16 = jnp.bfloat16
SIDE = 4
HEADS = 8
HD = 128
TOK = 128
GROUP = 2 * SIDE * SIDE
QS = 4
KVR = 264
STR = 24
DOCS = 8
UNROLL = 4
FAR = 1 << 20
LOG2E = 1.4426950408889634

FIRST_OUT = (
    ("z", 0, 0, 0, 0), ("z", 0, 0, 0, 1), ("t", 0, 0, 0, 0), ("t", 0, 0, 1, 1),
    ("d", 0, 0, 0, 0), ("d", 0, 0, 1, 1), ("d", 0, 0, 0, 1), ("d", 0, 0, 1, 0),
    ("s", 0, 0, 0, 0), ("s", 0, 0, 1, 1), ("s", 0, 0, 0, 1), ("s", 0, 0, 1, 0),
)
THEN_OUT = (
    ("t", 1, 0, 0, 0), ("s", 1, 0, 1, 0), ("d", 1, 0, 0, 0), ("d", 1, 0, 1, 0),
    ("g", 0, 0, 1, 1), ("d", 1, 0, 1, 1), ("d", 1, 0, 0, 1), ("s", 1, 0, 0, 0),
    ("t", 1, 0, 1, 1), ("r", 0, 0, 0, 0), ("s", 1, 0, 0, 1), ("d", 0, 2, 0, 0),
    ("s", 1, 0, 1, 1), ("d", 1, 2, 0, 0), ("d", 1, 2, 1, 0), ("d", 0, 2, 0, 1),
    ("g", 1, 0, 0, 0), ("d", 0, 2, 1, 1), ("g", 1, 0, 1, 1), ("d", 0, 1, 0, 0),
    ("d", 1, 1, 0, 0), ("d", 0, 2, 1, 0), ("d", 1, 1, 1, 0), ("r", 1, 0, 0, 0),
    ("d", 0, 3, 0, 0), ("d", 1, 3, 0, 0), ("d", 0, 1, 1, 1), ("d", 1, 1, 1, 1),
    ("g", 0, 0, 0, 0), ("d", 1, 1, 0, 1), ("d", 0, 3, 1, 1), ("d", 1, 2, 1, 1),
    ("g", 0, 2, 0, 0), ("g", 1, 2, 0, 0), ("d", 0, 1, 1, 0), ("d", 1, 3, 1, 1),
    ("d", 0, 1, 0, 1), ("d", 1, 2, 0, 1), ("g", 0, 2, 1, 1), ("r", 2, 0, 0, 0),
    ("d", 1, 3, 1, 0), ("g", 0, 1, 0, 0), ("g", 1, 1, 0, 0), ("d", 0, 3, 1, 0),
    ("g", 0, 3, 0, 0), ("g", 1, 1, 1, 1), ("g", 1, 3, 0, 0), ("g", 0, 1, 1, 1),
    ("d", 0, 3, 0, 1), ("g", 1, 2, 1, 1), ("d", 1, 3, 0, 1), ("g", 0, 3, 1, 1),
    ("g", 1, 3, 1, 1), ("r", 3, 0, 0, 0), ("r", 4, 0, 0, 0),
)
TERMS_OUT = (
    ("h", 1, 1, 1), ("h", 1, 1, 0), ("h", 0, 1, 1), ("h", 0, 1, 0), ("h", 1, 1, 3),
    ("h", 1, 1, 2), ("h", 0, 1, 2), ("h", 0, 1, 3), ("h", 1, 0, 0), ("h", 1, 0, 1),
    ("h", 0, 0, 0), ("h", 0, 0, 3), ("h", 1, 0, 2), ("h", 1, 0, 3), ("h", 0, 0, 1),
    ("h", 0, 0, 2), ("h", 1, 2, 1), ("h", 1, 2, 0), ("h", 0, 2, 0), ("h", 0, 2, 1),
    ("h", 1, 1, 5), ("h", 1, 1, 4), ("h", 0, 1, 5), ("h", 0, 1, 4), ("h", 1, 2, 2),
    ("h", 1, 2, 3), ("h", 0, 2, 2), ("h", 0, 2, 3), ("h", 1, 0, 5), ("h", 1, 0, 4),
    ("h", 0, 0, 4), ("h", 0, 3, 1), ("h", 0, 0, 5), ("h", 1, 3, 0), ("h", 1, 3, 1),
    ("h", 0, 3, 0), ("h", 1, 2, 5), ("h", 1, 2, 4), ("h", 0, 2, 5), ("h", 0, 2, 4),
    ("n", 1, 1, 0), ("n", 0, 1, 0), ("h", 1, 3, 3), ("h", 0, 3, 3), ("t", 1, 0, 1),
    ("t", 1, 0, 0), ("h", 1, 3, 2), ("h", 1, 3, 5), ("h", 1, 3, 4), ("n", 1, 2, 0),
    ("t", 0, 0, 1), ("t", 0, 0, 0), ("h", 0, 3, 4), ("h", 0, 3, 2), ("n", 0, 2, 0),
    ("h", 0, 3, 5), ("x", 1, 0, 0), ("x", 1, 0, 1),
)


class Place:
    def __init__(self):
        pb, ka = lax.axis_index("pb"), lax.axis_index("ka")
        self.c, self.zh = lax.rem(pb, 2), pb // 2
        self.zl, u = lax.rem(ka, 2), ka // 2
        self.x, self.y = u // SIDE, lax.rem(u, SIDE)
        self.z = self.zh * 2 + self.zl
        self.half = (1 - self.zl, self.zl)
        self.sib = self.dev(self.x, self.y, self.z, 1 - self.c)
        self.zq = self.dev(self.x, self.y, self.zh * 2 + 1 - self.zl, self.c)
        self.zk = self.dev(self.x, self.y, lax.rem(self.z + 3 + 2 * self.zl, SIDE), self.c)

    def dev(self, x, y, z, c):
        return {"pb": (z // 2) * 2 + c, "ka": (x * SIDE + y) * 2 + lax.rem(z, 2)}

    def moved(self, w, dp, ds):
        hw = self.half[w]
        x = lax.rem(self.x + SIDE + dp * (1 - hw) + ds * hw, SIDE)
        y = lax.rem(self.y + SIDE + dp * hw + ds * (1 - hw), SIDE)
        return x, y

    def nbr(self, w, dp, ds):
        x, y = self.moved(w, dp, ds)
        return self.dev(x, y, self.z, self.c)

    def slot(self, w, dp, ds):
        x, y = self.moved(w, dp, ds)
        return (x * SIDE + y) * 2 + self.half[w]

    def greet(self):
        partners = [
            self.sib,
            self.zq,
            self.zk,
            self.nbr(0, 1, 0),
            self.nbr(0, -1, 0),
            self.nbr(0, 0, 1),
            self.nbr(0, 0, -1),
            self.nbr(0, 2, 0),
            self.nbr(0, 0, 2),
        ]
        barrier = pltpu.get_barrier_semaphore()
        for partner in partners:
            pl.semaphore_signal(barrier, inc=1, device_id=partner, device_id_type=MESH)
        pl.semaphore_wait(barrier, len(partners))


def remote(src, dst, send_sem, recv_sem, device):
    return pltpu.make_async_remote_copy(
        src_ref=src,
        dst_ref=dst,
        send_sem=send_sem,
        recv_sem=recv_sem,
        device_id=device,
        device_id_type=MESH,
    )


def gather_kernel(
    q_in, k_in, v_in, o_in, g_in, lse_in, pos_in, seg_in,
    q_all, g_all, st_all, kv_all, dq_zero, dkv_zero,
    o_buf, lse_buf, pos_buf, seg_buf, loc, ksend, krecv, qsend, qrecv,
):
    at = Place()
    slot = at.slot(0, 0, 0)
    qslot = at.zl * 2 + at.c
    local = [
        pltpu.make_async_copy(k_in, kv_all.at[slot, pl.ds(0, TOK)], loc.at[0]),
        pltpu.make_async_copy(v_in, kv_all.at[slot, pl.ds(TOK, TOK)], loc.at[1]),
        pltpu.make_async_copy(q_in, q_all.at[qslot], loc.at[2]),
        pltpu.make_async_copy(g_in, g_all.at[qslot], loc.at[3]),
        pltpu.make_async_copy(o_in, o_buf, loc.at[4]),
        pltpu.make_async_copy(lse_in, lse_buf, loc.at[5]),
        pltpu.make_async_copy(pos_in, pos_buf, loc.at[6]),
        pltpu.make_async_copy(seg_in, seg_buf, loc.at[7]),
    ]
    for copy in (local[6], local[7], *local[:6]):
        copy.start()
    at.greet()
    local[6].wait()
    local[7].wait()
    seg = seg_buf[...].astype(F32)
    pos = pos_buf[...].astype(F32)
    row = lax.broadcasted_iota(jnp.int32, (KVR - 2 * TOK, TOK), 0)
    block_number = (pos_buf[...] // TOK).astype(F32)
    kv_all[slot, pl.ds(2 * TOK, KVR - 2 * TOK), :] = jnp.where(row == 0, seg, block_number).astype(BF16)
    sends, arrived = [], set()
    numbers = {m: n for n, m in enumerate(m for m in FIRST_OUT + THEN_OUT if m[0] != "r")}
    columns = (0, -1, 1, 2)

    def route(m):
        kind, w, j, d, h = m
        way = 1 - 2 * d
        if kind == "z":
            return slot, at.slot(1, 0, 0), at.zk
        if kind == "s":
            return at.slot(w, 0, 0), at.slot(w, -way, 0), at.nbr(w, way, 0)
        if kind == "t":
            return at.slot(w, 0, 0), at.slot(w, 2, 0), at.nbr(w, 2, 0)
        dp = columns[j]
        if kind == "d":
            return at.slot(w, dp, 0), at.slot(w, dp, -way), at.nbr(w, 0, way)
        return at.slot(w, dp, -way), at.slot(w, dp, 2), at.nbr(w, 0, way)

    def needs(m):
        kind, w, j, d, h = m
        if kind == "g":
            return ("d", w, j, h, h)
        if kind == "d" and j > 0:
            return (None, ("s", w, 0, 0, h), ("s", w, 0, 1, h), ("t", w, 0, h, h))[j]
        return ("z", 0, 0, 0, h) if w == 1 else None

    def kv_copy(m, where, device):
        part = kv_all.at[where, pl.ds(0, TOK) if m[4] == 0 else pl.ds(TOK, KVR - TOK)]
        return remote(part, part, ksend.at[numbers[m]], krecv.at[numbers[m]], device)

    def go(copy):
        copy.start()
        sends.append(copy)

    def arrive(m):
        if m not in arrived:
            arrived.add(m)
            _, where, device = route(m)
            kv_copy(m, where, device).wait_recv()

    def send(m):
        if needs(m):
            arrive(needs(m))
        where, _, device = route(m)
        go(kv_copy(m, where, device))

    def piece(who, n):
        if n < 4:
            ref = q_all if n < 2 else g_all
            return ref.at[who, pl.ds((n % 2) * (TOK // 2), TOK // 2)]
        return st_all.at[who]

    def q_copy(kind, n, who, device):
        part = piece(who, n)
        return remote(part, part, qsend.at[5 * kind + n], qrecv.at[5 * kind + n], device)

    local[0].wait()
    local[1].wait()
    for m in FIRST_OUT:
        send(m)
    local[2].wait()
    for n in (0, 1):
        go(q_copy(0, n, qslot, at.zq))
    local[3].wait()
    for n in (2, 3):
        go(q_copy(0, n, qslot, at.zq))
    for n in range(4):
        go(q_copy(1, n, qslot, at.sib))

    local[4].wait()
    local[5].wait()
    st_all[qslot, pl.ds(0, HEADS), :] = lse_buf[...]
    for h in range(HEADS):
        cols = pl.ds(h * HD, HD)
        prod = g_all[qslot, :, cols].astype(F32) * o_buf[:, cols].astype(F32)
        st_all[qslot, pl.ds(HEADS + h, 1), :] = jnp.sum(prod.T, axis=0, keepdims=True)
    row = lax.broadcasted_iota(jnp.int32, (8, TOK), 0)
    st_all[qslot, pl.ds(16, 8), :] = jnp.where(row == 0, seg, pos)
    dq_zero[...] = jnp.zeros_like(dq_zero)
    dkv_zero[...] = jnp.zeros_like(dkv_zero)
    go(q_copy(0, 4, qslot, at.zq))
    go(q_copy(1, 4, qslot, at.sib))

    far = (1 - at.zl) * 2 + at.c
    for m in THEN_OUT:
        if m[0] == "r":
            q_copy(0, m[1], far, at.zq).wait_recv()
            go(q_copy(2, m[1], far, at.sib))
        else:
            send(m)
    for m in numbers:
        arrive(m)
    for n in range(5):
        q_copy(1, n, at.zl * 2 + 1 - at.c, at.sib).wait_recv()
        q_copy(2, n, (1 - at.zl) * 2 + 1 - at.c, at.sib).wait_recv()
    for copy in sends:
        copy.wait_send()


def grads_kernel(
    q_ref, g_ref, st_ref, kv_ref, dq_zero, dkv_zero, dq_ref, dkv_ref,
    listed, low_ref, base_ref, bias_ref, w_buf, s_buf,
):
    tail = kv_ref[:, pl.ds(2 * TOK, KVR - 2 * TOK), :].astype(F32)
    key_doc = tail[:, 0, :].astype(jnp.int32)
    key_base = tail[:, 1, :].astype(jnp.int32) * TOK
    base_ref[...] = key_base
    lane = lax.broadcasted_iota(jnp.int32, (GROUP, TOK), 1)
    key_place = key_base + lane
    query_doc = jnp.concatenate([st_ref[i, pl.ds(16, 1), :] for i in range(QS)], axis=0)
    query_doc = query_doc.astype(jnp.int32)
    query_place = jnp.concatenate([st_ref[i, pl.ds(17, 1), :] for i in range(QS)], axis=0)
    query_place = query_place.astype(jnp.int32)
    low = jnp.full((QS, TOK), FAR, jnp.int32)
    for d in range(DOCS):
        first = jnp.where(key_doc == d, key_place, FAR)
        first = jnp.min(jnp.min(first, axis=0, keepdims=True), axis=1, keepdims=True)
        low = jnp.where(query_doc == d, first, low)
    low_ref[pl.ds(0, QS), :] = low
    low_ref[pl.ds(QS, QS), :] = query_place
    key_row = lax.broadcasted_iota(jnp.int32, (GROUP, TOK), 0)
    count = jnp.int32(0)
    for i in range(QS):
        top = jnp.max(query_place[i : i + 1], axis=1, keepdims=True)
        least = jnp.min(low[i : i + 1], axis=1, keepdims=True)
        active = (key_base <= top) & (key_base + (TOK - 1) >= least)
        for part in range(2):
            bits = jnp.where(
                active & (key_row // 16 == part), jnp.left_shift(1, lax.rem(key_row, 16)), 0
            )
            word = jnp.max(jnp.sum(bits, axis=0, keepdims=True))

            def note(j, count, i=i, part=part, word=word):
                listed[count] = i * 64 + (part * 16 + j) * 2 + 1
                return count + (lax.shift_right_logical(word, j) & 1)

            for j in range(16):
                count = note(j, count)
        last = listed[jnp.maximum(count - 1, 0)]
        listed[count] = last & -2
        count = count + (count & 1)

    sublane = lax.broadcasted_iota(jnp.int32, (TOK, TOK), 0)
    score_scale = HD ** (-0.5) * LOG2E
    nt = (((1,), (1,)), ((), ()))


    w_buf[...] = jnp.zeros_like(w_buf)
    s_buf[...] = jnp.zeros_like(s_buf)

    def late(i, k0, k1):
        kk = jnp.concatenate([kv_ref[k0, pl.ds(0, TOK), :], kv_ref[k1, pl.ds(0, TOK), :]], axis=0)
        kt = kk.T

        stack_g = jnp.concatenate([g_ref[i, :, pl.ds(h * HD, HD)] for h in range(HEADS)], axis=0)
        stack_q = jnp.concatenate([q_ref[i, :, pl.ds(h * HD, HD)] for h in range(HEADS)], axis=0)

        dv = jnp.dot(w_buf[...], stack_g, preferred_element_type=F32)
        dk = jnp.dot(s_buf[...], stack_q, preferred_element_type=F32)

        dkv_ref[k0, pl.ds(0, TOK), :] += dk[:TOK]
        dkv_ref[k0, pl.ds(TOK, TOK), :] += dv[:TOK]
        dkv_ref[k1, pl.ds(0, TOK), :] += dk[TOK:]
        dkv_ref[k1, pl.ds(TOK, TOK), :] += dv[TOK:]

        dq_ref[i] += jnp.dot(kt, s_buf[...], preferred_element_type=F32)

    def over_pairs(pair, before):
        late(*before)
        one, two = listed[2 * pair], listed[2 * pair + 1]
        i = one // 64
        k0 = lax.rem(one // 2, GROUP)
        k1 = lax.rem(two // 2, GROUP)
        lo, hi = low_ref[pl.ds(i, 1), :], low_ref[pl.ds(QS + i, 1), :]
        b0, b1 = base_ref[pl.ds(k0, 1), :], base_ref[pl.ds(k1, 1), :]
        hi1 = jnp.where((two & 1) == 1, hi - b1, -1)
        bias_ref[pl.ds(0, TOK), :] = jnp.where(
            (sublane >= lo - b0) & (sublane <= hi - b0), 0.0, -1e30
        )
        bias_ref[pl.ds(TOK, TOK), :] = jnp.where(
            (sublane >= lo - b1) & (sublane <= hi1), 0.0, -1e30
        )
        kk = jnp.concatenate([kv_ref[k0, pl.ds(0, TOK), :], kv_ref[k1, pl.ds(0, TOK), :]], axis=0)
        vv = jnp.concatenate(
            [kv_ref[k0, pl.ds(TOK, TOK), :], kv_ref[k1, pl.ds(TOK, TOK), :]], axis=0
        )

        def heads(ref, hp):
            a = ref[i, :, pl.ds(2 * hp * HD, HD)]
            b = ref[i, :, pl.ds((2 * hp + 1) * HD, HD)]
            return jnp.concatenate([a, b], axis=0)

        def rows(first, hp):
            a = st_ref[i, pl.ds(first + 2 * hp, 1), :]
            b = st_ref[i, pl.ds(first + 2 * hp + 1, 1), :]
            return jnp.concatenate([a, b], axis=1)

        for hp in range(HEADS // 2):
            cols = pl.ds(2 * hp * HD, 2 * HD)
            hs = range(2 * hp, 2 * hp + 2)
            qh = jnp.concatenate([q_ref[i, :, pl.ds(h * HD, HD)] for h in hs], axis=0)
            gh = jnp.concatenate([g_ref[i, :, pl.ds(h * HD, HD)] for h in hs], axis=0)
            lse = jnp.concatenate([st_ref[i, pl.ds(h, 1), :] for h in hs], axis=1)
            delta = jnp.concatenate([st_ref[i, pl.ds(HEADS + h, 1), :] for h in hs], axis=1)
            scores = lax.dot_general(kk, qh, nt, preferred_element_type=F32)
            bias = bias_ref[...]
            bias = jnp.concatenate([bias] * 2, axis=1)
            weights = jnp.exp2(scores * score_scale + (bias - lse * LOG2E))
            w_buf[:, cols] = weights.astype(BF16)
            grads = lax.dot_general(vv, gh, nt, preferred_element_type=F32)
            s_buf[:, cols] = (weights * (grads - delta)).astype(BF16)
        return i, k0, k1

    def several(turn, before):
        for n in range(UNROLL):
            before = over_pairs(spare + turn * UNROLL + n, before)
        return before

    pairs = count // 2
    spare = lax.rem(pairs, UNROLL)
    start = lax.fori_loop(0, spare, over_pairs, (jnp.int32(0),) * 3)
    late(*lax.fori_loop(0, pairs // UNROLL, several, start))


def reduce_kernel(
    dq_ref, dkv_ref,
    dq_out, dk_out, dv_out,
    out1, in1, out2, in2, out3, in3, near, sibq, farq_out, farq_in,
    s1, r1, s2, r2, s3, r3, sq, rq,
):
    at = Place()
    score_scale = HD ** (-0.5)
    sends = []

    def go(copy):
        copy.start()
        sends.append(copy)

    at.greet()
    qslot = at.zl * 2 + at.c
    sib_far = (1 - at.zl) * 2 + 1 - at.c
    sib_own = at.zl * 2 + 1 - at.c
    my_far = (1 - at.zl) * 2 + at.c
    CH = HD // 4

    def far_piece(n):
        rows = pl.ds(n * CH, CH)
        return remote(dq_ref.at[sib_far, rows], near.at[rows], sq.at[n], rq.at[n], at.sib)

    def far_send(n):
        rows = pl.ds(n * CH, CH)
        return remote(farq_out.at[rows], farq_in.at[rows], sq.at[4 + n], rq.at[4 + n], at.zq)

    own_piece = remote(dq_ref.at[sib_own], sibq, sq.at[8], rq.at[8], at.sib)
    for n in range(4):
        go(far_piece(n))
    go(own_piece)

    order = (2, 1, -1, 0)
    K, V = pl.ds(0, HD), pl.ds(HD, HD)

    def hop1(w, j, t):
        ahead = 1 if t % 2 == 0 else -1
        n = (w * 4 + j) * 6 + t
        return remote(out1.at[n], in1.at[n], s1.at[n], r1.at[n], at.nbr(w, 0, ahead))

    def first(w, j, t):
        where = (2, 2, 1, -1, 1, -1)[t]
        rows = (K, V, V, K, K, V)[t]
        value = dkv_ref[at.slot(w, order[j], where), rows, :]
        n = (w * 4 + j) * 6 + t
        if t >= 4:
            hop1(w, j, t - 4).wait_recv()
            value = value + in1[n - 4].astype(F32)
        out1[n] = value.astype(BF16)
        go(hop1(w, j, t))

    def settle(w, j):
        base = (w * 4 + j) * 6
        for t in (2, 3, 4, 5):
            hop1(w, j, t).wait_recv()
        own = dkv_ref[at.slot(w, order[j], 0)]
        dk = own[:HD] + in1[base + 3].astype(F32) + in1[base + 4].astype(F32)
        dv = own[HD:] + in1[base + 2].astype(F32) + in1[base + 5].astype(F32)
        return dk, dv

    def whole(w, j):
        n = w * 3 + j
        return remote(out2.at[n], in2.at[n], s2.at[4 + n], r2.at[4 + n], at.nbr(w, order[j], 0))

    def side(w, t):
        n = w * 3
        return remote(
            out2.at[n, t], in2.at[n, t], s2.at[2 * w + t], r2.at[2 * w + t], at.nbr(w, 2, 0)
        )

    def total(w):
        dk, dv = settle(w, 3)
        for t in (0, 1):
            side(w, t).wait_recv()
        for j in (1, 2):
            whole(w, j).wait_recv()
        for j in (0, 1, 2):
            dk = dk + in2[w * 3 + j, 0].astype(F32)
            dv = dv + in2[w * 3 + j, 1].astype(F32)
        return dk, dv

    def far(n):
        rows = pl.ds(n * CH, CH)
        far_piece(n).wait_recv()
        farq_out[rows, :] = (dq_ref[my_far, rows, :] + near[rows, :]).astype(BF16)
        go(far_send(n))

    across = [remote(out3.at[n], in3.at[n], s3.at[n], r3.at[n], at.zk) for n in range(2)]
    known = {}

    def sums(w, j):
        if (w, j) not in known:
            known[w, j] = total(w) if j == 3 else settle(w, j)
        return known[w, j]

    for n, (kind, w, j, t) in enumerate(TERMS_OUT):
        if n in (16, 18, 20, 22):
            far((n - 16) // 2)
        if kind == "h":
            first(w, j, t)
        elif kind == "t":
            out2[w * 3, t] = sums(w, 0)[t].astype(BF16)
            go(side(w, t))
        elif kind == "n":
            dk, dv = sums(w, j)
            out2[w * 3 + j, 0] = dk.astype(BF16)
            out2[w * 3 + j, 1] = dv.astype(BF16)
            go(whole(w, j))
        else:
            out3[t] = sums(1, 3)[t].astype(BF16)
            go(across[t])
    own_piece.wait_recv()
    for n in range(4):
        far_send(n).wait_recv()
    for h in range(HEADS):
        cols = pl.ds(h * HD, HD)
        value = dq_ref[qslot, :, cols] + sibq[:, cols] + farq_in[:, cols].astype(F32)
        dq_out[:, cols] = (value * score_scale).T.astype(BF16)
    dk, dv = total(0)
    across[0].wait_recv()
    dk_out[...] = ((dk + in3[0].astype(F32)) * score_scale).astype(BF16)
    across[1].wait_recv()
    dv_out[...] = (dv + in3[1].astype(F32)).astype(BF16)
    for copy in sends:
        copy.wait_send()


def store_kernel(dq_in, dk_in, dv_in, dq_out, dk_out, dv_out, sem):
    copies = [
        pltpu.make_async_copy(dq_in, dq_out, sem.at[0]),
        pltpu.make_async_copy(dk_in, dk_out, sem.at[1]),
        pltpu.make_async_copy(dv_in, dv_out, sem.at[2]),
    ]
    for copy in copies:
        copy.start()
    for copy in copies:
        copy.wait()


HB = pl.BlockSpec(memory_space=pltpu.HBM)
VM = pl.BlockSpec(memory_space=pltpu.VMEM)
DMA = pltpu.SemaphoreType.DMA


def gather(queries, key_rows, value_rows, forward_out, out_grad, logsumexp, position, segment):
    wide = HEADS * HD
    args = (
        queries, key_rows, value_rows, forward_out, out_grad,
        logsumexp, position.reshape(1, TOK), segment.reshape(1, TOK),
    )
    return pl.pallas_call(
        gather_kernel,
        out_shape=(
            pltpu.VMEM((QS, TOK, wide), BF16),
            pltpu.VMEM((QS, TOK, wide), BF16),
            pltpu.VMEM((QS, STR, TOK), F32),
            pltpu.VMEM((GROUP, KVR, HD), BF16),
            pltpu.VMEM((QS, HD, wide), F32),
            pltpu.VMEM((GROUP, 2 * HD, HD), F32),
        ),
        in_specs=[HB] * 8,
        out_specs=(VM,) * 6,
        scratch_shapes=[
            pltpu.VMEM((TOK, wide), BF16),
            pltpu.VMEM((HEADS, TOK), F32),
            pltpu.VMEM((1, TOK), jnp.int32),
            pltpu.VMEM((1, TOK), jnp.int32),
            DMA((8,)),
            DMA((62,)),
            DMA((62,)),
            DMA((15,)),
            DMA((15,)),
        ],
        compiler_params=pltpu.CompilerParams(
            collective_id=0, has_side_effects=True, vmem_limit_bytes=8 << 20
        ),
        name="gather_rows",
    )(*[pltpu.with_memory_space_constraint(a, pltpu.HBM) for a in args])


def grads(q_all, g_all, st_all, kv_all, dq_zero, dkv_zero):
    wide = HEADS * HD
    return pl.pallas_call(
        grads_kernel,
        out_shape=(
            pltpu.VMEM((QS, HD, wide), F32),
            pltpu.VMEM((GROUP, 2 * HD, HD), F32),
        ),
        in_specs=[VM] * 6,
        out_specs=(VM,) * 2,
        input_output_aliases={4: 0, 5: 1},
        scratch_shapes=[
            pltpu.SMEM((QS * GROUP + 16,), jnp.int32),
            pltpu.VMEM((2 * QS, TOK), jnp.int32),
            pltpu.VMEM((GROUP, TOK), jnp.int32),
            pltpu.VMEM((2 * TOK, TOK), F32),
            pltpu.VMEM((2 * TOK, wide), BF16),
            pltpu.VMEM((2 * TOK, wide), BF16),
        ],
        compiler_params=pltpu.CompilerParams(vmem_limit_bytes=24 << 20),
        name="tile_grads",
    )(q_all, g_all, st_all, kv_all, dq_zero, dkv_zero)


def reduce(dq_all, dkv_all):
    wide = HEADS * HD
    return pl.pallas_call(
        reduce_kernel,
        out_shape=(
            pltpu.VMEM((TOK, wide), BF16),
            pltpu.VMEM((TOK, HD), BF16),
            pltpu.VMEM((TOK, HD), BF16),
        ),
        in_specs=[VM] * 2,
        out_specs=(VM,) * 3,
        scratch_shapes=[
            pltpu.VMEM((48, HD, HD), BF16),
            pltpu.VMEM((48, HD, HD), BF16),
            pltpu.VMEM((6, 2, HD, HD), BF16),
            pltpu.VMEM((6, 2, HD, HD), BF16),
            pltpu.VMEM((2, HD, HD), BF16),
            pltpu.VMEM((2, HD, HD), BF16),
            pltpu.VMEM((HD, wide), F32),
            pltpu.VMEM((HD, wide), F32),
            pltpu.VMEM((HD, wide), BF16),
            pltpu.VMEM((HD, wide), BF16),
            DMA((48,)), DMA((48,)), DMA((10,)), DMA((10,)), DMA((2,)), DMA((2,)), DMA((9,)), DMA((9,)),
        ],
        compiler_params=pltpu.CompilerParams(
            collective_id=1, has_side_effects=True, vmem_limit_bytes=24 << 20
        ),
        name="reduce_grads",
    )(dq_all, dkv_all)


def store(dq, dk, dv):
    return pl.pallas_call(
        store_kernel,
        out_shape=tuple(pltpu.HBM(a.shape, BF16) for a in (dq, dk, dv)),
        in_specs=[VM] * 3,
        out_specs=(HB,) * 3,
        scratch_shapes=[DMA((3,))],
        name="store_grads",
    )(*[pltpu.with_memory_space_constraint(a, pltpu.VMEM) for a in (dq, dk, dv)])


def body(*args):
    return store(*reduce(*grads(*gather(*args))))


def solution(mesh):
    rows = P(("pb", "ka"), None)
    flat = P(("pb", "ka"))
    placed = (rows,) * 5 + (P(None, ("pb", "ka")), flat, flat)
    return jax.shard_map(
        body, mesh=mesh, in_specs=placed, out_specs=(rows,) * 3, check_vma=False
    )
```

```python
import functools

import jax
import jax.numpy as jnp
from jax import lax
from jax.experimental import pallas as pl
from jax.experimental.pallas import tpu as pltpu
from jax.sharding import PartitionSpec as P

MESH = pl.DeviceIdType.MESH
F32 = jnp.float32
BF16 = jnp.bfloat16
SIDE = 4
HEADS = 8
HD = 128
TOK = 128
GROUP = 2 * SIDE * SIDE
QS = 4
KVR = 264
STR = 24
DOCS = 8
UNROLL = 4
FAR = 1 << 20
LOG2E = 1.4426950408889634

FIRST_OUT = (
    ("z", 0, 0, 0, 2), ("s", 0, 0, 0, 2), ("s", 0, 0, 1, 2), ("d", 0, 0, 0, 2),
    ("d", 0, 0, 1, 2), ("t", 0, 0, 0, 0), ("t", 0, 0, 1, 1),
)
THEN_OUT = (
    ("s", 1, 0, 0, 2), ("s", 1, 0, 1, 2), ("d", 1, 0, 0, 2), ("d", 1, 0, 1, 2),
    ("r", 0, 0, 0, 0), ("t", 1, 0, 0, 0), ("t", 1, 0, 1, 1), ("d", 0, 1, 0, 2),
    ("d", 0, 1, 1, 2), ("d", 1, 1, 0, 2), ("d", 1, 1, 1, 2), ("r", 1, 0, 0, 0),
    ("d", 0, 3, 0, 2), ("d", 0, 3, 1, 2), ("d", 1, 2, 0, 2), ("d", 1, 2, 1, 2),
    ("d", 0, 2, 0, 2), ("d", 0, 2, 1, 2), ("d", 1, 3, 0, 2), ("d", 1, 3, 1, 2),
    ("r", 2, 0, 0, 0), ("g", 0, 1, 0, 0), ("g", 0, 1, 1, 1), ("g", 0, 0, 0, 0),
    ("g", 0, 0, 1, 1), ("g", 1, 1, 0, 0), ("g", 1, 1, 1, 1), ("g", 0, 3, 0, 0),
    ("g", 1, 0, 0, 0), ("g", 0, 3, 1, 1), ("g", 1, 0, 1, 1), ("r", 3, 0, 0, 0),
    ("g", 1, 2, 0, 0), ("g", 0, 2, 0, 0), ("g", 1, 2, 1, 1), ("g", 0, 2, 1, 1),
    ("r", 4, 0, 0, 0), ("g", 1, 3, 0, 0), ("g", 1, 3, 1, 1),
)
TERMS_OUT = (
    ("h", 1, 1, 1), ("h", 1, 1, 0), ("h", 0, 1, 1), ("h", 0, 1, 0), ("h", 1, 1, 3),
    ("h", 1, 1, 2), ("h", 0, 1, 2), ("h", 0, 1, 3), ("h", 1, 0, 0), ("h", 1, 0, 1),
    ("h", 0, 0, 0), ("h", 0, 0, 3), ("h", 1, 0, 2), ("h", 1, 0, 3), ("h", 0, 0, 1),
    ("h", 0, 0, 2), ("h", 1, 2, 1), ("h", 1, 2, 0), ("h", 0, 2, 0), ("h", 0, 2, 1),
    ("h", 1, 1, 5), ("h", 1, 1, 4), ("h", 0, 1, 5), ("h", 0, 1, 4), ("h", 1, 2, 2),
    ("h", 1, 2, 3), ("h", 0, 2, 2), ("h", 0, 2, 3), ("h", 1, 0, 5), ("h", 1, 0, 4),
    ("h", 0, 0, 4), ("h", 0, 3, 1), ("h", 0, 0, 5), ("h", 1, 3, 0), ("h", 1, 3, 1),
    ("h", 0, 3, 0), ("h", 1, 2, 5), ("h", 1, 2, 4), ("h", 0, 2, 5), ("h", 0, 2, 4),
    ("n", 1, 1, 0), ("n", 0, 1, 0), ("h", 1, 3, 3), ("h", 0, 3, 3), ("t", 1, 0, 1),
    ("t", 1, 0, 0), ("h", 1, 3, 2), ("h", 1, 3, 5), ("h", 1, 3, 4), ("n", 1, 2, 0),
    ("t", 0, 0, 1), ("t", 0, 0, 0), ("h", 0, 3, 4), ("h", 0, 3, 2), ("n", 0, 2, 0),
    ("h", 0, 3, 5), ("x", 1, 0, 0), ("x", 1, 0, 1),
)


class Place:
    def __init__(self):
        pb, ka = lax.axis_index("pb"), lax.axis_index("ka")
        self.c, self.zh = lax.rem(pb, 2), pb // 2
        self.zl, u = lax.rem(ka, 2), ka // 2
        self.x, self.y = u // SIDE, lax.rem(u, SIDE)
        self.z = self.zh * 2 + self.zl
        self.half = (1 - self.zl, self.zl)
        self.sib = self.dev(self.x, self.y, self.z, 1 - self.c)
        self.zq = self.dev(self.x, self.y, self.zh * 2 + 1 - self.zl, self.c)
        self.zk = self.dev(self.x, self.y, lax.rem(self.z + 3 + 2 * self.zl, SIDE), self.c)

    def dev(self, x, y, z, c):
        return {"pb": (z // 2) * 2 + c, "ka": (x * SIDE + y) * 2 + lax.rem(z, 2)}

    def moved(self, w, dp, ds):
        hw = self.half[w]
        x = lax.rem(self.x + SIDE + dp * (1 - hw) + ds * hw, SIDE)
        y = lax.rem(self.y + SIDE + dp * hw + ds * (1 - hw), SIDE)
        return x, y

    def nbr(self, w, dp, ds):
        x, y = self.moved(w, dp, ds)
        return self.dev(x, y, self.z, self.c)

    def slot(self, w, dp, ds):
        x, y = self.moved(w, dp, ds)
        return (x * SIDE + y) * 2 + self.half[w]

    def greet(self):
        partners = [
            self.sib,
            self.zq,
            self.zk,
            self.nbr(0, 1, 0),
            self.nbr(0, -1, 0),
            self.nbr(0, 0, 1),
            self.nbr(0, 0, -1),
            self.nbr(0, 2, 0),
            self.nbr(0, 0, 2),
        ]
        barrier = pltpu.get_barrier_semaphore()
        for partner in partners:
            pl.semaphore_signal(barrier, inc=1, device_id=partner, device_id_type=MESH)
        return lambda: pl.semaphore_wait(barrier, len(partners))


def remote(src, dst, send_sem, recv_sem, device):
    return pltpu.make_async_remote_copy(
        src_ref=src,
        dst_ref=dst,
        send_sem=send_sem,
        recv_sem=recv_sem,
        device_id=device,
        device_id_type=MESH,
    )


def gather_kernel(
    q_in, k_in, v_in, o_in, g_in, lse_in, pos_in, seg_in,
    q_all, g_all, st_all, kv_all, dq_zero, dkv_zero,
    o_buf, lse_buf, pos_buf, seg_buf, loc, ksend, krecv, qsend, qrecv,
):
    at = Place()
    slot = at.slot(0, 0, 0)
    qslot = at.zl * 2 + at.c
    local = [
        pltpu.make_async_copy(k_in, kv_all.at[slot, pl.ds(0, TOK)], loc.at[0]),
        pltpu.make_async_copy(v_in, kv_all.at[slot, pl.ds(TOK, TOK)], loc.at[1]),
        pltpu.make_async_copy(q_in, q_all.at[qslot], loc.at[2]),
        pltpu.make_async_copy(g_in, g_all.at[qslot], loc.at[3]),
        pltpu.make_async_copy(o_in, o_buf, loc.at[4]),
        pltpu.make_async_copy(lse_in, lse_buf, loc.at[5]),
        pltpu.make_async_copy(pos_in, pos_buf, loc.at[6]),
        pltpu.make_async_copy(seg_in, seg_buf, loc.at[7]),
    ]
    for copy in (local[6], local[7], *local[:6]):
        copy.start()
    everyone_here = at.greet()
    local[6].wait()
    local[7].wait()
    seg = seg_buf[...].astype(F32)
    pos = pos_buf[...].astype(F32)
    row = lax.broadcasted_iota(jnp.int32, (KVR - 2 * TOK, TOK), 0)
    block_number = (pos_buf[...] // TOK).astype(F32)
    kv_all[slot, pl.ds(2 * TOK, KVR - 2 * TOK), :] = jnp.where(row == 0, seg, block_number).astype(BF16)
    sends, arrived = [], set()
    numbers = {m: n for n, m in enumerate(m for m in FIRST_OUT + THEN_OUT if m[0] != "r")}
    columns = (0, -1, 1, 2)

    def route(m):
        kind, w, j, d, h = m
        way = 1 - 2 * d
        if kind == "z":
            return slot, at.slot(1, 0, 0), at.zk
        if kind == "s":
            return at.slot(w, 0, 0), at.slot(w, -way, 0), at.nbr(w, way, 0)
        if kind == "t":
            return at.slot(w, 0, 0), at.slot(w, 2, 0), at.nbr(w, 2, 0)
        dp = columns[j]
        if kind == "d":
            return at.slot(w, dp, 0), at.slot(w, dp, -way), at.nbr(w, 0, way)
        return at.slot(w, dp, -way), at.slot(w, dp, 2), at.nbr(w, 0, way)

    def needs(m):
        kind, w, j, d, h = m
        if kind == "g":
            return (("d", w, j, h, 2),)
        if kind == "d" and j == 3:
            return ("t", w, 0, 0, 0), ("t", w, 0, 1, 1)
        if kind == "d" and j > 0:
            return (("s", w, 0, j - 1, 2),)
        return (("z", 0, 0, 0, 2),) if w == 1 else ()

    def kv_copy(m, where, device):
        rows = (pl.ds(0, TOK), pl.ds(TOK, KVR - TOK), pl.ds(0, KVR))[m[4]]
        part = kv_all.at[where, rows]
        return remote(part, part, ksend.at[numbers[m]], krecv.at[numbers[m]], device)

    def go(copy):
        copy.start()
        sends.append(copy)

    def arrive(m):
        if m not in arrived:
            arrived.add(m)
            _, where, device = route(m)
            kv_copy(m, where, device).wait_recv()

    def send(m):
        for other in needs(m):
            arrive(other)
        where, _, device = route(m)
        go(kv_copy(m, where, device))

    def piece(who, n):
        if n < 4:
            ref = q_all if n < 2 else g_all
            return ref.at[who, pl.ds((n % 2) * (TOK // 2), TOK // 2)]
        return st_all.at[who]

    def q_copy(kind, n, who, device):
        part = piece(who, n)
        return remote(part, part, qsend.at[5 * kind + n], qrecv.at[5 * kind + n], device)

    local[0].wait()
    local[1].wait()
    everyone_here()
    for m in FIRST_OUT:
        send(m)
    local[2].wait()
    for n in (0, 1):
        go(q_copy(0, n, qslot, at.zq))
    local[3].wait()
    for n in (2, 3):
        go(q_copy(0, n, qslot, at.zq))
    for n in range(4):
        go(q_copy(1, n, qslot, at.sib))

    local[4].wait()
    local[5].wait()
    st_all[qslot, pl.ds(0, HEADS), :] = lse_buf[...]
    for h in range(HEADS):
        cols = pl.ds(h * HD, HD)
        prod = g_all[qslot, :, cols].astype(F32) * o_buf[:, cols].astype(F32)
        st_all[qslot, pl.ds(HEADS + h, 1), :] = jnp.sum(prod.T, axis=0, keepdims=True)
    row = lax.broadcasted_iota(jnp.int32, (8, TOK), 0)
    st_all[qslot, pl.ds(16, 8), :] = jnp.where(row == 0, seg, pos)
    dq_zero[...] = jnp.zeros_like(dq_zero)
    dkv_zero[...] = jnp.zeros_like(dkv_zero)
    go(q_copy(0, 4, qslot, at.zq))
    go(q_copy(1, 4, qslot, at.sib))

    far = (1 - at.zl) * 2 + at.c
    for m in THEN_OUT:
        if m[0] == "r":
            q_copy(0, m[1], far, at.zq).wait_recv()
            go(q_copy(2, m[1], far, at.sib))
        else:
            send(m)
    for n in range(5):
        q_copy(1, n, at.zl * 2 + 1 - at.c, at.sib).wait_recv()
    for copy in sends:
        copy.wait_send()
    for m in numbers:
        arrive(m)
    for n in range(5):
        q_copy(2, n, (1 - at.zl) * 2 + 1 - at.c, at.sib).wait_recv()


def grads_kernel(
    q_ref, g_ref, st_ref, kv_ref, dq_zero, dkv_zero, dq_ref, dkv_ref,
    listed, low_ref, base_ref, bias_ref, w_buf, s_buf,
):
    tail = kv_ref[:, pl.ds(2 * TOK, KVR - 2 * TOK), :].astype(F32)
    key_doc = tail[:, 0, :].astype(jnp.int32)
    key_base = tail[:, 1, :].astype(jnp.int32) * TOK
    base_ref[...] = key_base
    lane = lax.broadcasted_iota(jnp.int32, (GROUP, TOK), 1)
    key_place = key_base + lane
    query_doc = jnp.concatenate([st_ref[i, pl.ds(16, 1), :] for i in range(QS)], axis=0)
    query_doc = query_doc.astype(jnp.int32)
    query_place = jnp.concatenate([st_ref[i, pl.ds(17, 1), :] for i in range(QS)], axis=0)
    query_place = query_place.astype(jnp.int32)
    low = jnp.full((QS, TOK), FAR, jnp.int32)
    for d in range(DOCS):
        first = jnp.where(key_doc == d, key_place, FAR)
        first = jnp.min(jnp.min(first, axis=0, keepdims=True), axis=1, keepdims=True)
        low = jnp.where(query_doc == d, first, low)
    low_ref[pl.ds(0, QS), :] = low
    low_ref[pl.ds(QS, QS), :] = query_place
    key_row = lax.broadcasted_iota(jnp.int32, (GROUP, TOK), 0)
    count = jnp.int32(0)
    for i in range(QS):
        top = jnp.max(query_place[i : i + 1], axis=1, keepdims=True)
        least = jnp.min(low[i : i + 1], axis=1, keepdims=True)
        active = (key_base <= top) & (key_base + (TOK - 1) >= least)
        for part in range(2):
            bits = jnp.where(
                active & (key_row // 16 == part), jnp.left_shift(1, lax.rem(key_row, 16)), 0
            )
            word = jnp.max(jnp.sum(bits, axis=0, keepdims=True))

            def note(j, count, i=i, part=part, word=word):
                listed[count] = i * 64 + (part * 16 + j) * 2 + 1
                return count + (lax.shift_right_logical(word, j) & 1)

            for j in range(16):
                count = note(j, count)
        last = listed[jnp.maximum(count - 1, 0)]
        listed[count] = last & -2
        count = count + (count & 1)

    sublane = lax.broadcasted_iota(jnp.int32, (TOK, TOK), 0)
    score_scale = HD ** (-0.5) * LOG2E
    nt = (((1,), (1,)), ((), ()))


    w_buf[...] = jnp.zeros_like(w_buf)
    s_buf[...] = jnp.zeros_like(s_buf)

    def late(i, k0, k1):
        kk = jnp.concatenate([kv_ref[k0, pl.ds(0, TOK), :], kv_ref[k1, pl.ds(0, TOK), :]], axis=0)
        kt = kk.T

        stack_g = jnp.concatenate([g_ref[i, :, pl.ds(h * HD, HD)] for h in range(HEADS)], axis=0)
        stack_q = jnp.concatenate([q_ref[i, :, pl.ds(h * HD, HD)] for h in range(HEADS)], axis=0)

        dv = jnp.dot(w_buf[...], stack_g, preferred_element_type=F32)
        dk = jnp.dot(s_buf[...], stack_q, preferred_element_type=F32)

        dkv_ref[k0, pl.ds(0, TOK), :] += dk[:TOK]
        dkv_ref[k0, pl.ds(TOK, TOK), :] += dv[:TOK]
        dkv_ref[k1, pl.ds(0, TOK), :] += dk[TOK:]
        dkv_ref[k1, pl.ds(TOK, TOK), :] += dv[TOK:]

        dq_ref[i] += jnp.dot(kt, s_buf[...], preferred_element_type=F32)

    def over_pairs(pair, before):
        late(*before)
        one, two = listed[2 * pair], listed[2 * pair + 1]
        i = one // 64
        k0 = lax.rem(one // 2, GROUP)
        k1 = lax.rem(two // 2, GROUP)
        lo, hi = low_ref[pl.ds(i, 1), :], low_ref[pl.ds(QS + i, 1), :]
        b0, b1 = base_ref[pl.ds(k0, 1), :], base_ref[pl.ds(k1, 1), :]
        hi1 = jnp.where((two & 1) == 1, hi - b1, -1)
        bias_ref[pl.ds(0, TOK), :] = jnp.where(
            (sublane >= lo - b0) & (sublane <= hi - b0), 0.0, -1e30
        )
        bias_ref[pl.ds(TOK, TOK), :] = jnp.where(
            (sublane >= lo - b1) & (sublane <= hi1), 0.0, -1e30
        )
        kk = jnp.concatenate([kv_ref[k0, pl.ds(0, TOK), :], kv_ref[k1, pl.ds(0, TOK), :]], axis=0)
        vv = jnp.concatenate(
            [kv_ref[k0, pl.ds(TOK, TOK), :], kv_ref[k1, pl.ds(TOK, TOK), :]], axis=0
        )

        def heads(ref, hp):
            a = ref[i, :, pl.ds(2 * hp * HD, HD)]
            b = ref[i, :, pl.ds((2 * hp + 1) * HD, HD)]
            return jnp.concatenate([a, b], axis=0)

        def rows(first, hp):
            a = st_ref[i, pl.ds(first + 2 * hp, 1), :]
            b = st_ref[i, pl.ds(first + 2 * hp + 1, 1), :]
            return jnp.concatenate([a, b], axis=1)

        for hp in range(HEADS // 2):
            cols = pl.ds(2 * hp * HD, 2 * HD)
            hs = range(2 * hp, 2 * hp + 2)
            qh = jnp.concatenate([q_ref[i, :, pl.ds(h * HD, HD)] for h in hs], axis=0)
            gh = jnp.concatenate([g_ref[i, :, pl.ds(h * HD, HD)] for h in hs], axis=0)
            lse = jnp.concatenate([st_ref[i, pl.ds(h, 1), :] for h in hs], axis=1)
            delta = jnp.concatenate([st_ref[i, pl.ds(HEADS + h, 1), :] for h in hs], axis=1)
            scores = lax.dot_general(kk, qh, nt, preferred_element_type=F32)
            bias = bias_ref[...]
            bias = jnp.concatenate([bias] * 2, axis=1)
            weights = jnp.exp2(scores * score_scale + (bias - lse * LOG2E))
            w_buf[:, cols] = weights.astype(BF16)
            grads = lax.dot_general(vv, gh, nt, preferred_element_type=F32)
            s_buf[:, cols] = (weights * (grads - delta)).astype(BF16)
        return i, k0, k1

    def several(turn, before):
        for n in range(UNROLL):
            before = over_pairs(spare + turn * UNROLL + n, before)
        return before

    pairs = count // 2
    spare = lax.rem(pairs, UNROLL)
    start = lax.fori_loop(0, spare, over_pairs, (jnp.int32(0),) * 3)
    late(*lax.fori_loop(0, pairs // UNROLL, several, start))


def reduce_kernel(
    dq_ref, dkv_ref,
    dq_out, dk_out, dv_out,
    out1, in1, out2, in2, out3, in3, near, sibq, farq_out, farq_in,
    s1, r1, s2, r2, s3, r3, sq, rq,
):
    at = Place()
    score_scale = HD ** (-0.5)
    sends = []

    def go(copy):
        copy.start()
        sends.append(copy)

    at.greet()()
    qslot = at.zl * 2 + at.c
    sib_far = (1 - at.zl) * 2 + 1 - at.c
    sib_own = at.zl * 2 + 1 - at.c
    my_far = (1 - at.zl) * 2 + at.c
    CH = HD // 4

    def far_piece(n):
        rows = pl.ds(n * CH, CH)
        return remote(dq_ref.at[sib_far, rows], near.at[rows], sq.at[n], rq.at[n], at.sib)

    def far_send(n):
        rows = pl.ds(n * CH, CH)
        return remote(farq_out.at[rows], farq_in.at[rows], sq.at[4 + n], rq.at[4 + n], at.zq)

    own_piece = remote(dq_ref.at[sib_own], sibq, sq.at[8], rq.at[8], at.sib)
    for n in range(4):
        go(far_piece(n))
    go(own_piece)

    order = (2, 1, -1, 0)
    K, V = pl.ds(0, HD), pl.ds(HD, HD)

    def hop1(w, j, t):
        ahead = 1 if t % 2 == 0 else -1
        n = (w * 4 + j) * 6 + t
        return remote(out1.at[n], in1.at[n], s1.at[n], r1.at[n], at.nbr(w, 0, ahead))

    def first(w, j, t):
        where = (2, 2, 1, -1, 1, -1)[t]
        rows = (K, V, V, K, K, V)[t]
        value = dkv_ref[at.slot(w, order[j], where), rows, :]
        n = (w * 4 + j) * 6 + t
        if t >= 4:
            hop1(w, j, t - 4).wait_recv()
            value = value + in1[n - 4].astype(F32)
        out1[n] = value.astype(BF16)
        go(hop1(w, j, t))

    def settle(w, j):
        base = (w * 4 + j) * 6
        for t in (2, 3, 4, 5):
            hop1(w, j, t).wait_recv()
        own = dkv_ref[at.slot(w, order[j], 0)]
        dk = own[:HD] + in1[base + 3].astype(F32) + in1[base + 4].astype(F32)
        dv = own[HD:] + in1[base + 2].astype(F32) + in1[base + 5].astype(F32)
        return dk, dv

    def whole(w, j):
        n = w * 3 + j
        return remote(out2.at[n], in2.at[n], s2.at[4 + n], r2.at[4 + n], at.nbr(w, order[j], 0))

    def side(w, t):
        n = w * 3
        return remote(
            out2.at[n, t], in2.at[n, t], s2.at[2 * w + t], r2.at[2 * w + t], at.nbr(w, 2, 0)
        )

    def total(w):
        dk, dv = settle(w, 3)
        for t in (0, 1):
            side(w, t).wait_recv()
        for j in (1, 2):
            whole(w, j).wait_recv()
        for j in (0, 1, 2):
            dk = dk + in2[w * 3 + j, 0].astype(F32)
            dv = dv + in2[w * 3 + j, 1].astype(F32)
        return dk, dv

    def far(n):
        rows = pl.ds(n * CH, CH)
        far_piece(n).wait_recv()
        farq_out[rows, :] = (dq_ref[my_far, rows, :] + near[rows, :]).astype(BF16)
        go(far_send(n))

    across = [remote(out3.at[n], in3.at[n], s3.at[n], r3.at[n], at.zk) for n in range(2)]
    known = {}

    def sums(w, j):
        if (w, j) not in known:
            known[w, j] = total(w) if j == 3 else settle(w, j)
        return known[w, j]

    for n, (kind, w, j, t) in enumerate(TERMS_OUT):
        if n in (16, 18, 20, 22):
            far((n - 16) // 2)
        if kind == "h":
            first(w, j, t)
        elif kind == "t":
            out2[w * 3, t] = sums(w, 0)[t].astype(BF16)
            go(side(w, t))
        elif kind == "n":
            dk, dv = sums(w, j)
            out2[w * 3 + j, 0] = dk.astype(BF16)
            out2[w * 3 + j, 1] = dv.astype(BF16)
            go(whole(w, j))
        else:
            out3[t] = sums(1, 3)[t].astype(BF16)
            go(across[t])
    own_piece.wait_recv()
    for n in range(4):
        far_send(n).wait_recv()
    for h in range(HEADS):
        cols = pl.ds(h * HD, HD)
        value = dq_ref[qslot, :, cols] + sibq[:, cols] + farq_in[:, cols].astype(F32)
        dq_out[:, cols] = (value * score_scale).T.astype(BF16)
    for copy in sends:
        copy.wait_send()
    dk, dv = total(0)
    across[0].wait_recv()
    dk_out[...] = ((dk + in3[0].astype(F32)) * score_scale).astype(BF16)
    across[1].wait_recv()
    dv_out[...] = (dv + in3[1].astype(F32)).astype(BF16)


def store_kernel(dq_in, dk_in, dv_in, dq_out, dk_out, dv_out, sem):
    copies = [
        pltpu.make_async_copy(dq_in, dq_out, sem.at[0]),
        pltpu.make_async_copy(dk_in, dk_out, sem.at[1]),
        pltpu.make_async_copy(dv_in, dv_out, sem.at[2]),
    ]
    for copy in copies:
        copy.start()
    for copy in copies:
        copy.wait()


HB = pl.BlockSpec(memory_space=pltpu.HBM)
VM = pl.BlockSpec(memory_space=pltpu.VMEM)
DMA = pltpu.SemaphoreType.DMA


def gather(queries, key_rows, value_rows, forward_out, out_grad, logsumexp, position, segment):
    wide = HEADS * HD
    args = (
        queries, key_rows, value_rows, forward_out, out_grad,
        logsumexp, position.reshape(1, TOK), segment.reshape(1, TOK),
    )
    return pl.pallas_call(
        gather_kernel,
        out_shape=(
            pltpu.VMEM((QS, TOK, wide), BF16),
            pltpu.VMEM((QS, TOK, wide), BF16),
            pltpu.VMEM((QS, STR, TOK), F32),
            pltpu.VMEM((GROUP, KVR, HD), BF16),
            pltpu.VMEM((QS, HD, wide), F32),
            pltpu.VMEM((GROUP, 2 * HD, HD), F32),
        ),
        in_specs=[HB] * 8,
        out_specs=(VM,) * 6,
        scratch_shapes=[
            pltpu.VMEM((TOK, wide), BF16),
            pltpu.VMEM((HEADS, TOK), F32),
            pltpu.VMEM((1, TOK), jnp.int32),
            pltpu.VMEM((1, TOK), jnp.int32),
            DMA((8,)),
            DMA((41,)),
            DMA((41,)),
            DMA((15,)),
            DMA((15,)),
        ],
        compiler_params=pltpu.CompilerParams(
            collective_id=0, has_side_effects=True, vmem_limit_bytes=8 << 20
        ),
        name="gather_rows",
    )(*[pltpu.with_memory_space_constraint(a, pltpu.HBM) for a in args])


def grads(q_all, g_all, st_all, kv_all, dq_zero, dkv_zero):
    wide = HEADS * HD
    return pl.pallas_call(
        grads_kernel,
        out_shape=(
            pltpu.VMEM((QS, HD, wide), F32),
            pltpu.VMEM((GROUP, 2 * HD, HD), F32),
        ),
        in_specs=[VM] * 6,
        out_specs=(VM,) * 2,
        input_output_aliases={4: 0, 5: 1},
        scratch_shapes=[
            pltpu.SMEM((QS * GROUP + 16,), jnp.int32),
            pltpu.VMEM((2 * QS, TOK), jnp.int32),
            pltpu.VMEM((GROUP, TOK), jnp.int32),
            pltpu.VMEM((2 * TOK, TOK), F32),
            pltpu.VMEM((2 * TOK, wide), BF16),
            pltpu.VMEM((2 * TOK, wide), BF16),
        ],
        compiler_params=pltpu.CompilerParams(vmem_limit_bytes=24 << 20),
        name="tile_grads",
    )(q_all, g_all, st_all, kv_all, dq_zero, dkv_zero)


def reduce(dq_all, dkv_all):
    wide = HEADS * HD
    return pl.pallas_call(
        reduce_kernel,
        out_shape=(
            pltpu.VMEM((TOK, wide), BF16),
            pltpu.VMEM((TOK, HD), BF16),
            pltpu.VMEM((TOK, HD), BF16),
        ),
        in_specs=[VM] * 2,
        out_specs=(VM,) * 3,
        scratch_shapes=[
            pltpu.VMEM((48, HD, HD), BF16),
            pltpu.VMEM((48, HD, HD), BF16),
            pltpu.VMEM((6, 2, HD, HD), BF16),
            pltpu.VMEM((6, 2, HD, HD), BF16),
            pltpu.VMEM((2, HD, HD), BF16),
            pltpu.VMEM((2, HD, HD), BF16),
            pltpu.VMEM((HD, wide), F32),
            pltpu.VMEM((HD, wide), F32),
            pltpu.VMEM((HD, wide), BF16),
            pltpu.VMEM((HD, wide), BF16),
            DMA((48,)), DMA((48,)), DMA((10,)), DMA((10,)), DMA((2,)), DMA((2,)), DMA((9,)), DMA((9,)),
        ],
        compiler_params=pltpu.CompilerParams(
            collective_id=1, has_side_effects=True, vmem_limit_bytes=24 << 20
        ),
        name="reduce_grads",
    )(dq_all, dkv_all)


def store(dq, dk, dv):
    return pl.pallas_call(
        store_kernel,
        out_shape=tuple(pltpu.HBM(a.shape, BF16) for a in (dq, dk, dv)),
        in_specs=[VM] * 3,
        out_specs=(HB,) * 3,
        scratch_shapes=[DMA((3,))],
        name="store_grads",
    )(*[pltpu.with_memory_space_constraint(a, pltpu.VMEM) for a in (dq, dk, dv)])


def body(*args):
    return store(*reduce(*grads(*gather(*args))))


def solution(mesh):
    rows = P(("pb", "ka"), None)
    flat = P(("pb", "ka"))
    placed = (rows,) * 5 + (P(None, ("pb", "ka")), flat, flat)
    return jax.shard_map(
        body, mesh=mesh, in_specs=placed, out_specs=(rows,) * 3, check_vma=False
    )
```

```python
import functools

import jax
import jax.numpy as jnp
from jax import lax
from jax.experimental import pallas as pl
from jax.experimental.pallas import tpu as pltpu
from jax.sharding import PartitionSpec as P

MESH = pl.DeviceIdType.MESH
F32 = jnp.float32
BF16 = jnp.bfloat16
SIDE = 4
HEADS = 8
HD = 128
TOK = 128
GROUP = 2 * SIDE * SIDE
QS = 4
KVR = 264
STR = 24
DOCS = 8
UNROLL = 6
FAR = 1 << 20
LOG2E = 1.4426950408889634

FIRST_OUT = (
    ("z", 0, 0, 0, 2), ("s", 0, 0, 0, 2), ("s", 0, 0, 1, 2), ("d", 0, 0, 0, 2),
    ("d", 0, 0, 1, 2), ("t", 0, 0, 0, 0), ("t", 0, 0, 1, 1),
)
THEN_OUT = (
    ("s", 1, 0, 0, 2), ("s", 1, 0, 1, 2), ("d", 1, 0, 0, 2), ("d", 1, 0, 1, 2),
    ("r", 0, 0, 0, 0), ("t", 1, 0, 0, 0), ("t", 1, 0, 1, 1), ("d", 0, 1, 0, 2),
    ("d", 0, 1, 1, 2), ("d", 1, 1, 0, 2), ("d", 1, 1, 1, 2), ("r", 1, 0, 0, 0),
    ("d", 0, 3, 0, 2), ("d", 0, 3, 1, 2), ("d", 1, 2, 0, 2), ("d", 1, 2, 1, 2),
    ("d", 0, 2, 0, 2), ("d", 0, 2, 1, 2), ("d", 1, 3, 0, 2), ("d", 1, 3, 1, 2),
    ("r", 2, 0, 0, 0), ("g", 0, 1, 0, 0), ("g", 0, 1, 1, 1), ("g", 0, 0, 0, 0),
    ("g", 0, 0, 1, 1), ("g", 1, 1, 0, 0), ("g", 1, 1, 1, 1), ("g", 0, 3, 0, 0),
    ("g", 1, 0, 0, 0), ("g", 0, 3, 1, 1), ("g", 1, 0, 1, 1), ("r", 3, 0, 0, 0),
    ("g", 1, 2, 0, 0), ("g", 0, 2, 0, 0), ("g", 1, 2, 1, 1), ("g", 0, 2, 1, 1),
    ("r", 4, 0, 0, 0), ("g", 1, 3, 0, 0), ("g", 1, 3, 1, 1),
)
TERMS_OUT = (
    ("h", 1, 1, 1), ("h", 1, 1, 0), ("h", 0, 1, 1), ("h", 0, 1, 0), ("h", 1, 1, 3),
    ("h", 1, 1, 2), ("h", 0, 1, 2), ("h", 0, 1, 3), ("h", 1, 0, 0), ("h", 1, 0, 1),
    ("h", 0, 0, 0), ("h", 0, 0, 3), ("h", 1, 0, 2), ("h", 1, 0, 3), ("h", 0, 0, 1),
    ("h", 0, 0, 2), ("h", 1, 2, 1), ("h", 1, 2, 0), ("h", 0, 2, 0), ("h", 0, 2, 1),
    ("h", 1, 1, 5), ("h", 1, 1, 4), ("h", 0, 1, 5), ("h", 0, 1, 4), ("h", 1, 2, 2),
    ("h", 1, 2, 3), ("h", 0, 2, 2), ("h", 0, 2, 3), ("h", 1, 0, 5), ("h", 1, 0, 4),
    ("h", 0, 0, 4), ("h", 0, 3, 1), ("h", 0, 0, 5), ("h", 1, 3, 0), ("h", 1, 3, 1),
    ("h", 0, 3, 0), ("h", 1, 2, 5), ("h", 1, 2, 4), ("h", 0, 2, 5), ("h", 0, 2, 4),
    ("n", 1, 1, 0), ("n", 0, 1, 0), ("h", 1, 3, 3), ("h", 0, 3, 3), ("t", 1, 0, 1),
    ("t", 1, 0, 0), ("h", 1, 3, 2), ("h", 1, 3, 5), ("h", 1, 3, 4), ("n", 1, 2, 0),
    ("t", 0, 0, 1), ("t", 0, 0, 0), ("h", 0, 3, 4), ("h", 0, 3, 2), ("n", 0, 2, 0),
    ("h", 0, 3, 5), ("x", 1, 0, 0), ("x", 1, 0, 1),
)


class Place:
    def __init__(self):
        pb, ka = lax.axis_index("pb"), lax.axis_index("ka")
        self.c, self.zh = lax.rem(pb, 2), pb // 2
        self.zl, u = lax.rem(ka, 2), ka // 2
        self.x, self.y = u // SIDE, lax.rem(u, SIDE)
        self.z = self.zh * 2 + self.zl
        self.half = (1 - self.zl, self.zl)
        self.sib = self.dev(self.x, self.y, self.z, 1 - self.c)
        self.zq = self.dev(self.x, self.y, self.zh * 2 + 1 - self.zl, self.c)
        self.zk = self.dev(self.x, self.y, lax.rem(self.z + 3 + 2 * self.zl, SIDE), self.c)

    def dev(self, x, y, z, c):
        return {"pb": (z // 2) * 2 + c, "ka": (x * SIDE + y) * 2 + lax.rem(z, 2)}

    def moved(self, w, dp, ds):
        hw = self.half[w]
        x = lax.rem(self.x + SIDE + dp * (1 - hw) + ds * hw, SIDE)
        y = lax.rem(self.y + SIDE + dp * hw + ds * (1 - hw), SIDE)
        return x, y

    def nbr(self, w, dp, ds):
        x, y = self.moved(w, dp, ds)
        return self.dev(x, y, self.z, self.c)

    def slot(self, w, dp, ds):
        x, y = self.moved(w, dp, ds)
        return (x * SIDE + y) * 2 + self.half[w]

    def greet(self):
        partners = [
            self.sib,
            self.zq,
            self.zk,
            self.nbr(0, 1, 0),
            self.nbr(0, -1, 0),
            self.nbr(0, 0, 1),
            self.nbr(0, 0, -1),
            self.nbr(0, 2, 0),
            self.nbr(0, 0, 2),
        ]
        barrier = pltpu.get_barrier_semaphore()
        for partner in partners:
            pl.semaphore_signal(barrier, inc=1, device_id=partner, device_id_type=MESH)
        return lambda: pl.semaphore_wait(barrier, len(partners))


def remote(src, dst, send_sem, recv_sem, device):
    return pltpu.make_async_remote_copy(
        src_ref=src,
        dst_ref=dst,
        send_sem=send_sem,
        recv_sem=recv_sem,
        device_id=device,
        device_id_type=MESH,
    )


def gather_kernel(
    q_in, k_in, v_in, o_in, g_in, lse_in, pos_in, seg_in,
    q_all, g_all, st_all, kv_all, dq_zero, dkv_zero,
    o_buf, lse_buf, pos_buf, seg_buf, loc, ksend, krecv, qsend, qrecv,
):
    at = Place()
    slot = at.slot(0, 0, 0)
    qslot = at.zl * 2 + at.c
    local = [
        pltpu.make_async_copy(k_in, kv_all.at[slot, pl.ds(0, TOK)], loc.at[0]),
        pltpu.make_async_copy(v_in, kv_all.at[slot, pl.ds(TOK, TOK)], loc.at[1]),
        pltpu.make_async_copy(q_in, q_all.at[qslot], loc.at[2]),
        pltpu.make_async_copy(g_in, g_all.at[qslot], loc.at[3]),
        pltpu.make_async_copy(o_in, o_buf, loc.at[4]),
        pltpu.make_async_copy(lse_in, lse_buf, loc.at[5]),
        pltpu.make_async_copy(pos_in, pos_buf, loc.at[6]),
        pltpu.make_async_copy(seg_in, seg_buf, loc.at[7]),
    ]
    for copy in (local[6], local[7], *local[:6]):
        copy.start()
    everyone_here = at.greet()
    local[6].wait()
    local[7].wait()
    seg = seg_buf[...].astype(F32)
    pos = pos_buf[...].astype(F32)
    row = lax.broadcasted_iota(jnp.int32, (KVR - 2 * TOK, TOK), 0)
    block_number = (pos_buf[...] // TOK).astype(F32)
    kv_all[slot, pl.ds(2 * TOK, KVR - 2 * TOK), :] = jnp.where(row == 0, seg, block_number).astype(BF16)
    sends, arrived = [], set()
    numbers = {m: n for n, m in enumerate(m for m in FIRST_OUT + THEN_OUT if m[0] != "r")}
    columns = (0, -1, 1, 2)

    def route(m):
        kind, w, j, d, h = m
        way = 1 - 2 * d
        if kind == "z":
            return slot, at.slot(1, 0, 0), at.zk
        if kind == "s":
            return at.slot(w, 0, 0), at.slot(w, -way, 0), at.nbr(w, way, 0)
        if kind == "t":
            return at.slot(w, 0, 0), at.slot(w, 2, 0), at.nbr(w, 2, 0)
        dp = columns[j]
        if kind == "d":
            return at.slot(w, dp, 0), at.slot(w, dp, -way), at.nbr(w, 0, way)
        return at.slot(w, dp, -way), at.slot(w, dp, 2), at.nbr(w, 0, way)

    def needs(m):
        kind, w, j, d, h = m
        if kind == "g":
            return (("d", w, j, h, 2),)
        if kind == "d" and j == 3:
            return ("t", w, 0, 0, 0), ("t", w, 0, 1, 1)
        if kind == "d" and j > 0:
            return (("s", w, 0, j - 1, 2),)
        return (("z", 0, 0, 0, 2),) if w == 1 else ()

    def kv_copy(m, where, device):
        rows = (pl.ds(0, TOK), pl.ds(TOK, KVR - TOK), pl.ds(0, KVR))[m[4]]
        part = kv_all.at[where, rows]
        return remote(part, part, ksend.at[numbers[m]], krecv.at[numbers[m]], device)

    def go(copy):
        copy.start()
        sends.append(copy)

    def arrive(m):
        if m not in arrived:
            arrived.add(m)
            _, where, device = route(m)
            kv_copy(m, where, device).wait_recv()

    def send(m):
        for other in needs(m):
            arrive(other)
        where, _, device = route(m)
        go(kv_copy(m, where, device))

    def piece(who, n):
        if n < 4:
            ref = q_all if n < 2 else g_all
            return ref.at[who, pl.ds((n % 2) * (TOK // 2), TOK // 2)]
        return st_all.at[who]

    def q_copy(kind, n, who, device):
        part = piece(who, n)
        return remote(part, part, qsend.at[5 * kind + n], qrecv.at[5 * kind + n], device)

    local[0].wait()
    local[1].wait()
    everyone_here()
    for m in FIRST_OUT:
        send(m)
    local[2].wait()
    for n in (0, 1):
        go(q_copy(0, n, qslot, at.zq))
    local[3].wait()
    for n in (2, 3):
        go(q_copy(0, n, qslot, at.zq))
    for n in range(4):
        go(q_copy(1, n, qslot, at.sib))

    local[4].wait()
    local[5].wait()
    st_all[qslot, pl.ds(0, HEADS), :] = lse_buf[...]
    for h in range(HEADS):
        cols = pl.ds(h * HD, HD)
        prod = g_all[qslot, :, cols].astype(F32) * o_buf[:, cols].astype(F32)
        st_all[qslot, pl.ds(HEADS + h, 1), :] = jnp.sum(prod.T, axis=0, keepdims=True)
    row = lax.broadcasted_iota(jnp.int32, (8, TOK), 0)
    st_all[qslot, pl.ds(16, 8), :] = jnp.where(row == 0, seg, pos)
    dq_zero[...] = jnp.zeros_like(dq_zero)
    dkv_zero[...] = jnp.zeros_like(dkv_zero)
    go(q_copy(0, 4, qslot, at.zq))
    go(q_copy(1, 4, qslot, at.sib))

    far = (1 - at.zl) * 2 + at.c
    for m in THEN_OUT:
        if m[0] == "r":
            q_copy(0, m[1], far, at.zq).wait_recv()
            go(q_copy(2, m[1], far, at.sib))
        else:
            send(m)
    for n in range(5):
        q_copy(1, n, at.zl * 2 + 1 - at.c, at.sib).wait_recv()
    for copy in sends:
        copy.wait_send()
    for m in numbers:
        arrive(m)
    for n in range(5):
        q_copy(2, n, (1 - at.zl) * 2 + 1 - at.c, at.sib).wait_recv()


def grads_kernel(
    q_ref, g_ref, st_ref, kv_ref, dq_zero, dkv_zero, dq_ref, dkv_ref,
    listed, low_ref, base_ref, bias_ref, w_buf, s_buf,
):
    tail = kv_ref[:, pl.ds(2 * TOK, KVR - 2 * TOK), :].astype(F32)
    key_doc = tail[:, 0, :].astype(jnp.int32)
    key_base = tail[:, 1, :].astype(jnp.int32) * TOK
    base_ref[...] = key_base
    lane = lax.broadcasted_iota(jnp.int32, (GROUP, TOK), 1)
    key_place = key_base + lane
    query_doc = jnp.concatenate([st_ref[i, pl.ds(16, 1), :] for i in range(QS)], axis=0)
    query_doc = query_doc.astype(jnp.int32)
    query_place = jnp.concatenate([st_ref[i, pl.ds(17, 1), :] for i in range(QS)], axis=0)
    query_place = query_place.astype(jnp.int32)
    low = jnp.full((QS, TOK), FAR, jnp.int32)
    for d in range(DOCS):
        first = jnp.where(key_doc == d, key_place, FAR)
        first = jnp.min(jnp.min(first, axis=0, keepdims=True), axis=1, keepdims=True)
        low = jnp.where(query_doc == d, first, low)
    low_ref[pl.ds(0, QS), :] = low
    low_ref[pl.ds(QS, QS), :] = query_place
    key_row = lax.broadcasted_iota(jnp.int32, (GROUP, TOK), 0)
    count = jnp.int32(0)
    for i in range(QS):
        top = jnp.max(query_place[i : i + 1], axis=1, keepdims=True)
        least = jnp.min(low[i : i + 1], axis=1, keepdims=True)
        active = (key_base <= top) & (key_base + (TOK - 1) >= least)
        for part in range(2):
            bits = jnp.where(
                active & (key_row // 16 == part), jnp.left_shift(1, lax.rem(key_row, 16)), 0
            )
            word = jnp.max(jnp.sum(bits, axis=0, keepdims=True))

            def note(j, count, i=i, part=part, word=word):
                listed[count] = i * 64 + (part * 16 + j) * 2 + 1
                return count + (lax.shift_right_logical(word, j) & 1)

            for j in range(16):
                count = note(j, count)
        last = listed[jnp.maximum(count - 1, 0)]
        listed[count] = last & -2
        count = count + (count & 1)

    sublane = lax.broadcasted_iota(jnp.int32, (TOK, TOK), 0)
    score_scale = HD ** (-0.5) * LOG2E
    nt = (((1,), (1,)), ((), ()))


    w_buf[...] = jnp.zeros_like(w_buf)
    s_buf[...] = jnp.zeros_like(s_buf)

    def late(i, k0, k1):
        kk = jnp.concatenate([kv_ref[k0, pl.ds(0, TOK), :], kv_ref[k1, pl.ds(0, TOK), :]], axis=0)
        kt = kk.T

        stack_g = jnp.concatenate([g_ref[i, :, pl.ds(h * HD, HD)] for h in range(HEADS)], axis=0)
        stack_q = jnp.concatenate([q_ref[i, :, pl.ds(h * HD, HD)] for h in range(HEADS)], axis=0)

        dv = jnp.dot(w_buf[...], stack_g, preferred_element_type=F32)
        dk = jnp.dot(s_buf[...], stack_q, preferred_element_type=F32)

        dkv_ref[k0, pl.ds(0, TOK), :] += dk[:TOK]
        dkv_ref[k0, pl.ds(TOK, TOK), :] += dv[:TOK]
        dkv_ref[k1, pl.ds(0, TOK), :] += dk[TOK:]
        dkv_ref[k1, pl.ds(TOK, TOK), :] += dv[TOK:]

        dq_ref[i] += jnp.dot(kt, s_buf[...], preferred_element_type=F32)

    def over_pairs(pair, before):
        late(*before)
        one, two = listed[2 * pair], listed[2 * pair + 1]
        i = one // 64
        k0 = lax.rem(one // 2, GROUP)
        k1 = lax.rem(two // 2, GROUP)
        lo, hi = low_ref[pl.ds(i, 1), :], low_ref[pl.ds(QS + i, 1), :]
        b0, b1 = base_ref[pl.ds(k0, 1), :], base_ref[pl.ds(k1, 1), :]
        hi1 = jnp.where((two & 1) == 1, hi - b1, -1)
        bias_ref[pl.ds(0, TOK), :] = jnp.where(
            (sublane >= lo - b0) & (sublane <= hi - b0), 0.0, -1e30
        )
        bias_ref[pl.ds(TOK, TOK), :] = jnp.where(
            (sublane >= lo - b1) & (sublane <= hi1), 0.0, -1e30
        )
        kk = jnp.concatenate([kv_ref[k0, pl.ds(0, TOK), :], kv_ref[k1, pl.ds(0, TOK), :]], axis=0)
        vv = jnp.concatenate(
            [kv_ref[k0, pl.ds(TOK, TOK), :], kv_ref[k1, pl.ds(TOK, TOK), :]], axis=0
        )

        def heads(ref, hp):
            a = ref[i, :, pl.ds(2 * hp * HD, HD)]
            b = ref[i, :, pl.ds((2 * hp + 1) * HD, HD)]
            return jnp.concatenate([a, b], axis=0)

        def rows(first, hp):
            a = st_ref[i, pl.ds(first + 2 * hp, 1), :]
            b = st_ref[i, pl.ds(first + 2 * hp + 1, 1), :]
            return jnp.concatenate([a, b], axis=1)

        for hp in range(HEADS // 2):
            cols = pl.ds(2 * hp * HD, 2 * HD)
            hs = range(2 * hp, 2 * hp + 2)
            qh = jnp.concatenate([q_ref[i, :, pl.ds(h * HD, HD)] for h in hs], axis=0)
            gh = jnp.concatenate([g_ref[i, :, pl.ds(h * HD, HD)] for h in hs], axis=0)
            lse = jnp.concatenate([st_ref[i, pl.ds(h, 1), :] for h in hs], axis=1)
            delta = jnp.concatenate([st_ref[i, pl.ds(HEADS + h, 1), :] for h in hs], axis=1)
            scores = lax.dot_general(kk, qh, nt, preferred_element_type=F32)
            bias = bias_ref[...]
            bias = jnp.concatenate([bias] * 2, axis=1)
            weights = jnp.exp2(scores * score_scale + (bias - lse * LOG2E))
            w_buf[:, cols] = weights.astype(BF16)
            grads = lax.dot_general(vv, gh, nt, preferred_element_type=F32)
            s_buf[:, cols] = (weights * (grads - delta)).astype(BF16)
        return i, k0, k1

    def several(turn, before):
        for n in range(UNROLL):
            before = over_pairs(spare + turn * UNROLL + n, before)
        return before

    pairs = count // 2
    spare = lax.rem(pairs, UNROLL)
    start = lax.fori_loop(0, spare, over_pairs, (jnp.int32(0),) * 3)
    late(*lax.fori_loop(0, pairs // UNROLL, several, start))


def reduce_kernel(
    dq_ref, dkv_ref,
    dq_out, dk_out, dv_out,
    out1, in1, out2, in2, out3, in3, near, sibq, farq_out, farq_in,
    s1, r1, s2, r2, s3, r3, sq, rq,
):
    at = Place()
    score_scale = HD ** (-0.5)
    sends = []

    def go(copy):
        copy.start()
        sends.append(copy)

    at.greet()()
    qslot = at.zl * 2 + at.c
    sib_far = (1 - at.zl) * 2 + 1 - at.c
    sib_own = at.zl * 2 + 1 - at.c
    my_far = (1 - at.zl) * 2 + at.c
    CH = HD // 4

    def far_piece(n):
        rows = pl.ds(n * CH, CH)
        return remote(dq_ref.at[sib_far, rows], near.at[rows], sq.at[n], rq.at[n], at.sib)

    def far_send(n):
        rows = pl.ds(n * CH, CH)
        return remote(farq_out.at[rows], farq_in.at[rows], sq.at[4 + n], rq.at[4 + n], at.zq)

    own_piece = remote(dq_ref.at[sib_own], sibq, sq.at[8], rq.at[8], at.sib)
    for n in range(4):
        go(far_piece(n))
    go(own_piece)

    order = (2, 1, -1, 0)
    K, V = pl.ds(0, HD), pl.ds(HD, HD)

    def hop1(w, j, t):
        ahead = 1 if t % 2 == 0 else -1
        n = (w * 4 + j) * 6 + t
        return remote(out1.at[n], in1.at[n], s1.at[n], r1.at[n], at.nbr(w, 0, ahead))

    def first(w, j, t):
        where = (2, 2, 1, -1, 1, -1)[t]
        rows = (K, V, V, K, K, V)[t]
        value = dkv_ref[at.slot(w, order[j], where), rows, :]
        n = (w * 4 + j) * 6 + t
        if t >= 4:
            hop1(w, j, t - 4).wait_recv()
            value = value + in1[n - 4].astype(F32)
        out1[n] = value.astype(BF16)
        go(hop1(w, j, t))

    def settle(w, j):
        base = (w * 4 + j) * 6
        for t in (2, 3, 4, 5):
            hop1(w, j, t).wait_recv()
        own = dkv_ref[at.slot(w, order[j], 0)]
        dk = own[:HD] + in1[base + 3].astype(F32) + in1[base + 4].astype(F32)
        dv = own[HD:] + in1[base + 2].astype(F32) + in1[base + 5].astype(F32)
        return dk, dv

    def whole(w, j):
        n = w * 3 + j
        return remote(out2.at[n], in2.at[n], s2.at[4 + n], r2.at[4 + n], at.nbr(w, order[j], 0))

    def side(w, t):
        n = w * 3
        return remote(
            out2.at[n, t], in2.at[n, t], s2.at[2 * w + t], r2.at[2 * w + t], at.nbr(w, 2, 0)
        )

    def total(w):
        dk, dv = settle(w, 3)
        for t in (0, 1):
            side(w, t).wait_recv()
        for j in (1, 2):
            whole(w, j).wait_recv()
        for j in (0, 1, 2):
            dk = dk + in2[w * 3 + j, 0].astype(F32)
            dv = dv + in2[w * 3 + j, 1].astype(F32)
        return dk, dv

    def far(n):
        rows = pl.ds(n * CH, CH)
        far_piece(n).wait_recv()
        farq_out[rows, :] = (dq_ref[my_far, rows, :] + near[rows, :]).astype(BF16)
        go(far_send(n))

    across = [remote(out3.at[n], in3.at[n], s3.at[n], r3.at[n], at.zk) for n in range(2)]
    known = {}

    def sums(w, j):
        if (w, j) not in known:
            known[w, j] = total(w) if j == 3 else settle(w, j)
        return known[w, j]

    for n, (kind, w, j, t) in enumerate(TERMS_OUT):
        if n in (16, 18, 20, 22):
            far((n - 16) // 2)
        if kind == "h":
            first(w, j, t)
        elif kind == "t":
            out2[w * 3, t] = sums(w, 0)[t].astype(BF16)
            go(side(w, t))
        elif kind == "n":
            dk, dv = sums(w, j)
            out2[w * 3 + j, 0] = dk.astype(BF16)
            out2[w * 3 + j, 1] = dv.astype(BF16)
            go(whole(w, j))
        else:
            out3[t] = sums(1, 3)[t].astype(BF16)
            go(across[t])
    own_piece.wait_recv()
    for n in range(4):
        far_send(n).wait_recv()
    for h in range(HEADS):
        cols = pl.ds(h * HD, HD)
        value = dq_ref[qslot, :, cols] + sibq[:, cols] + farq_in[:, cols].astype(F32)
        dq_out[:, cols] = (value * score_scale).T.astype(BF16)
    for copy in sends:
        copy.wait_send()
    dk, dv = total(0)
    across[0].wait_recv()
    dk_out[...] = ((dk + in3[0].astype(F32)) * score_scale).astype(BF16)
    across[1].wait_recv()
    dv_out[...] = (dv + in3[1].astype(F32)).astype(BF16)


def store_kernel(dq_in, dk_in, dv_in, dq_out, dk_out, dv_out, sem):
    copies = [
        pltpu.make_async_copy(dq_in, dq_out, sem.at[0]),
        pltpu.make_async_copy(dk_in, dk_out, sem.at[1]),
        pltpu.make_async_copy(dv_in, dv_out, sem.at[2]),
    ]
    for copy in copies:
        copy.start()
    for copy in copies:
        copy.wait()


HB = pl.BlockSpec(memory_space=pltpu.HBM)
VM = pl.BlockSpec(memory_space=pltpu.VMEM)
DMA = pltpu.SemaphoreType.DMA


def gather(queries, key_rows, value_rows, forward_out, out_grad, logsumexp, position, segment):
    wide = HEADS * HD
    args = (
        queries, key_rows, value_rows, forward_out, out_grad,
        logsumexp, position.reshape(1, TOK), segment.reshape(1, TOK),
    )
    return pl.pallas_call(
        gather_kernel,
        out_shape=(
            pltpu.VMEM((QS, TOK, wide), BF16),
            pltpu.VMEM((QS, TOK, wide), BF16),
            pltpu.VMEM((QS, STR, TOK), F32),
            pltpu.VMEM((GROUP, KVR, HD), BF16),
            pltpu.VMEM((QS, HD, wide), F32),
            pltpu.VMEM((GROUP, 2 * HD, HD), F32),
        ),
        in_specs=[HB] * 8,
        out_specs=(VM,) * 6,
        scratch_shapes=[
            pltpu.VMEM((TOK, wide), BF16),
            pltpu.VMEM((HEADS, TOK), F32),
            pltpu.VMEM((1, TOK), jnp.int32),
            pltpu.VMEM((1, TOK), jnp.int32),
            DMA((8,)),
            DMA((41,)),
            DMA((41,)),
            DMA((15,)),
            DMA((15,)),
        ],
        compiler_params=pltpu.CompilerParams(
            collective_id=0, has_side_effects=True, vmem_limit_bytes=8 << 20
        ),
        name="gather_rows",
    )(*[pltpu.with_memory_space_constraint(a, pltpu.HBM) for a in args])


def grads(q_all, g_all, st_all, kv_all, dq_zero, dkv_zero):
    wide = HEADS * HD
    return pl.pallas_call(
        grads_kernel,
        out_shape=(
            pltpu.VMEM((QS, HD, wide), F32),
            pltpu.VMEM((GROUP, 2 * HD, HD), F32),
        ),
        in_specs=[VM] * 6,
        out_specs=(VM,) * 2,
        input_output_aliases={4: 0, 5: 1},
        scratch_shapes=[
            pltpu.SMEM((QS * GROUP + 16,), jnp.int32),
            pltpu.VMEM((2 * QS, TOK), jnp.int32),
            pltpu.VMEM((GROUP, TOK), jnp.int32),
            pltpu.VMEM((2 * TOK, TOK), F32),
            pltpu.VMEM((2 * TOK, wide), BF16),
            pltpu.VMEM((2 * TOK, wide), BF16),
        ],
        compiler_params=pltpu.CompilerParams(vmem_limit_bytes=24 << 20),
        name="tile_grads",
    )(q_all, g_all, st_all, kv_all, dq_zero, dkv_zero)


def reduce(dq_all, dkv_all):
    wide = HEADS * HD
    return pl.pallas_call(
        reduce_kernel,
        out_shape=(
            pltpu.VMEM((TOK, wide), BF16),
            pltpu.VMEM((TOK, HD), BF16),
            pltpu.VMEM((TOK, HD), BF16),
        ),
        in_specs=[VM] * 2,
        out_specs=(VM,) * 3,
        scratch_shapes=[
            pltpu.VMEM((48, HD, HD), BF16),
            pltpu.VMEM((48, HD, HD), BF16),
            pltpu.VMEM((6, 2, HD, HD), BF16),
            pltpu.VMEM((6, 2, HD, HD), BF16),
            pltpu.VMEM((2, HD, HD), BF16),
            pltpu.VMEM((2, HD, HD), BF16),
            pltpu.VMEM((HD, wide), F32),
            pltpu.VMEM((HD, wide), F32),
            pltpu.VMEM((HD, wide), BF16),
            pltpu.VMEM((HD, wide), BF16),
            DMA((48,)), DMA((48,)), DMA((10,)), DMA((10,)), DMA((2,)), DMA((2,)), DMA((9,)), DMA((9,)),
        ],
        compiler_params=pltpu.CompilerParams(
            collective_id=1, has_side_effects=True, vmem_limit_bytes=24 << 20
        ),
        name="reduce_grads",
    )(dq_all, dkv_all)


def store(dq, dk, dv):
    return pl.pallas_call(
        store_kernel,
        out_shape=tuple(pltpu.HBM(a.shape, BF16) for a in (dq, dk, dv)),
        in_specs=[VM] * 3,
        out_specs=(HB,) * 3,
        scratch_shapes=[DMA((3,))],
        name="store_grads",
    )(*[pltpu.with_memory_space_constraint(a, pltpu.VMEM) for a in (dq, dk, dv)])


def body(*args):
    return store(*reduce(*grads(*gather(*args))))


def solution(mesh):
    rows = P(("pb", "ka"), None)
    flat = P(("pb", "ka"))
    placed = (rows,) * 5 + (P(None, ("pb", "ka")), flat, flat)
    return jax.shard_map(
        body, mesh=mesh, in_specs=placed, out_specs=(rows,) * 3, check_vma=False
    )
```
